512 devices in a mesh: group: 2 (over y), ha: 16 (over x, core), wa: 16 (over z).
Axes of the slice: x: 8, y: 2, z: 16, core: 2. Of those that a mesh axis runs over, the one named last changes fastest.
The devices are a block of a 8x8x16 slice.
Arguments:
- queries: bfloat16 [4, 128, 128, 1536], P('group', 'ha', 'wa'), parts along dimension 0, may hold values from -6 to 6
- keys: bfloat16 [4, 128, 128, 1536], P('group', 'ha', 'wa'), parts along dimension 0, may hold values from -6 to 6
- values: bfloat16 [4, 128, 128, 1536], P('group', 'ha', 'wa'), parts along dimension 0, may hold values from -6 to 6
- out_grad: bfloat16 [4, 128, 128, 1536], P('group', 'ha', 'wa'), parts along dimension 0, may hold values from -96 to 96
- log_norm: float32 [12, 4, 128, 128], P(None, 'group', 'ha', 'wa'), parts along dimension 1, may hold values from 6.5 to 7.5
- delta_rows: float32 [12, 4, 128, 128], P(None, 'group', 'ha', 'wa'), parts along dimension 1, may hold values from -360 to 360
- text_keys: bfloat16 [64, 1536], P('group'), parts along dimension 0, may hold values from -6 to 6
- text_values: bfloat16 [64, 1536], P('group'), parts along dimension 0, may hold values from -6 to 6
- window_table: int32 [16, 16, 9], replicated, may hold values 0 or 1
Outputs:
- query_grad: bfloat16 [4, 128, 128, 1536], P('group', 'ha', 'wa'), parts along dimension 0
- key_grad: bfloat16 [4, 128, 128, 1536], P('group', 'ha', 'wa'), parts along dimension 0
- value_grad: bfloat16 [4, 128, 128, 1536], P('group', 'ha', 'wa'), parts along dimension 0
- text_key_grad: bfloat16 [64, 1536], P('group'), parts along dimension 0
- text_value_grad: bfloat16 [64, 1536], P('group'), parts along dimension 0
The draws below stay inside these ranges and needn't reach their ends.
There are 2 independent parts, one for each index of `group`. The reference program is written for one: setup_inputs(seed, part) draws one part's arguments, and reference() takes and returns one part's arrays. A program takes and returns all parts, laid end to end along the dimension named above; an argument that names none is the same for every part. Nothing has to cross between parts.
All inputs are finite; a program needn't handle non-finite values.
Results may differ from the reference program's by a relative error of at most 0.001.
The reference program's roundings to bfloat16 on the way (of `probs_half` and `score_grad`) count: a program that leaves them out, or rounds other values in their place, can miss the bound.
Values may be sent and summed in bfloat16 or wider, within the bound.
A program may use at most 64 MiB of HBM per device.

```python
import jax
import jax.numpy as jnp
from jax import lax

HEADS = 12
HDIM = 128
TEXT = 32
FRAMES = 2
TILE = 8
HALO = 2
HD = 1536
NH = 128
NW = 128
N_HA = 16
N_WA = 16


def place_ends(array, own_key, least, high):
    place = [jax.random.randint(jax.random.fold_in(own_key, axis), (), 0, length) for axis, length in enumerate(array.shape)]
    longest = array.shape.index(max(array.shape))
    neighbour = place[:longest] + [(place[longest] + 1) % array.shape[longest]] + place[longest + 1:]
    return array.at[tuple(place)].set(least).at[tuple(neighbour)].set(high)


def shard_levels(stream_key, dims, split, least, largest):
    gain, own = 1.0, jax.random.fold_in(stream_key, 6)
    for axis_at, shards_of in split:
        heights = jnp.exp(jax.random.uniform(jax.random.fold_in(own, axis_at), (shards_of,), jnp.float32, least / len(split), largest / len(split)))
        gain = gain * jnp.repeat(heights, dims[axis_at] // shards_of).reshape([-1 if axis == axis_at else 1 for axis in range(len(dims))])
    return gain


def gaussian(rng, dims, scale, most, shards=(), kind=jnp.bfloat16):
    drawn = jax.random.normal(rng, dims, jnp.float32) * scale
    if len(shards) > 0:
        drawn = shard_levels(rng, dims, shards, -0.22, 0.18) * drawn
    return jnp.clip(drawn, min=-most, max=most).astype(kind)


def setup_inputs(seed: int = 0, part: int = 0) -> dict:
    streams_of = jax.random.split(jax.random.key(seed), 10)
    part_keys = jax.random.split(jax.random.fold_in(streams_of[9], part), 10)
    return {
        "queries": gaussian(part_keys[0], (FRAMES, NH, NW, HD), 1.0, 6.0, ((1, 16), (2, 16))),
        "keys": gaussian(part_keys[1], (FRAMES, NH, NW, HD), 1.0, 6.0, ((1, 16), (2, 16))),
        "values": gaussian(part_keys[2], (FRAMES, NH, NW, HD), 1.0, 6.0, ((1, 16), (2, 16))),
        "out_grad": gaussian(part_keys[3], (FRAMES, NH, NW, HD), 16.0, 96.0, ((1, 16), (2, 16))),
        "log_norm": jnp.clip(6.5 + 1.0 * jax.random.uniform(part_keys[4], (HEADS, FRAMES, NH, NW), jnp.float32) ** shard_levels(part_keys[4], (HEADS, FRAMES, NH, NW), ((2, 16), (3, 16)), -0.2, 0.2), 6.5, 7.5),
        "delta_rows": gaussian(part_keys[5], (HEADS, FRAMES, NH, NW), 60.0, 360.0, ((2, 16), (3, 16)), jnp.float32),
        "text_keys": gaussian(part_keys[6], (TEXT, HD), 1.0, 6.0),
        "text_values": gaussian(part_keys[7], (TEXT, HD), 1.0, 6.0),
        "window_table": place_ends((jax.random.randint(streams_of[8], (N_HA, N_WA, 9), 0, 4) < 3).astype(jnp.int32), jax.random.fold_in(streams_of[8], 1), 0, 1),
    }


def tile_grads(query_rows, cotangent_rows, norm_rows, delta_part, key_rows, value_rows, cell_mask):
    score_scale = 1.0 / (HDIM ** 0.5)
    query_wide = query_rows.astype(jnp.float32)
    cotangent_wide = cotangent_rows.astype(jnp.float32)
    key_wide = key_rows.astype(jnp.float32)
    value_wide = value_rows.astype(jnp.float32)
    scores = jnp.einsum("qhd,khd->hqk", query_wide, key_wide) * score_scale
    probs = jnp.exp(scores - norm_rows[:, :, None])
    if cell_mask is not None:
        probs = probs * cell_mask[None, None, :]
    probs_half = probs.astype(jnp.bfloat16)
    value_part = jnp.einsum("hqk,qhd->khd", probs_half.astype(jnp.float32), cotangent_wide)
    prob_grad = jnp.einsum("qhd,khd->hqk", cotangent_wide, value_wide)
    score_grad = (probs * (prob_grad - delta_part[:, :, None])).astype(jnp.bfloat16).astype(jnp.float32)
    query_part = jnp.einsum("hqk,khd->qhd", score_grad, key_wide) * score_scale
    key_part = jnp.einsum("hqk,qhd->khd", score_grad, query_wide) * score_scale
    return query_part, key_part, value_part


def reference(queries, keys, values, out_grad, log_norm, delta_rows, text_keys, text_values, window_table):
    frames, rows_all, cols_all, width = queries.shape
    tile_side = TILE
    halo_rim = HALO
    window_side = TILE + 2 * HALO
    pad_spec = ((0, 0), (halo_rim, halo_rim), (halo_rim, halo_rim), (0, 0))
    key_pad = jnp.pad(keys, pad_spec, mode="wrap")
    value_pad = jnp.pad(values, pad_spec, mode="wrap")
    position = jnp.arange(window_side, dtype=jnp.int32)
    block_of = (position >= halo_rim).astype(jnp.int32) + (position >= halo_rim + tile_side).astype(jnp.int32)
    text_key_rows = text_keys.reshape(TEXT, HEADS, HDIM)
    text_value_rows = text_values.reshape(TEXT, HEADS, HDIM)

    def per_tile(carry, tile_index):
        grad_pad, text_total = carry
        row_tile = (tile_index // N_WA).astype(jnp.int32)
        col_tile = (tile_index % N_WA).astype(jnp.int32)
        row_start = (row_tile * tile_side).astype(jnp.int32)
        col_start = (col_tile * tile_side).astype(jnp.int32)
        anchor = jnp.zeros((), jnp.int32)
        tile_shape = (frames, tile_side, tile_side, width)
        query_rows = lax.dynamic_slice(queries, (anchor, row_start, col_start, anchor), tile_shape).reshape(-1, HEADS, HDIM)
        cotangent_rows = lax.dynamic_slice(out_grad, (anchor, row_start, col_start, anchor), tile_shape).reshape(-1, HEADS, HDIM)
        stat_shape = (HEADS, frames, tile_side, tile_side)
        norm_rows = lax.dynamic_slice(log_norm, (anchor, anchor, row_start, col_start), stat_shape).reshape(HEADS, -1)
        delta_part = lax.dynamic_slice(delta_rows, (anchor, anchor, row_start, col_start), stat_shape).reshape(HEADS, -1)
        window_shape = (frames, window_side, window_side, width)
        key_rows = lax.dynamic_slice(key_pad, (anchor, row_start, col_start, anchor), window_shape).reshape(-1, HEADS, HDIM)
        value_rows = lax.dynamic_slice(value_pad, (anchor, row_start, col_start, anchor), window_shape).reshape(-1, HEADS, HDIM)
        pattern = lax.dynamic_slice(window_table, (row_tile, col_tile, anchor), (1, 1, 9)).reshape(9).astype(jnp.float32)
        cell_grid = pattern[3 * block_of[:, None] + block_of[None, :]]
        cell_mask = jnp.broadcast_to(cell_grid[None], (frames, window_side, window_side)).reshape(-1)
        video_query, video_key, video_value = tile_grads(query_rows, cotangent_rows, norm_rows, delta_part, key_rows, value_rows, cell_mask)
        text_query, text_key, text_value = tile_grads(query_rows, cotangent_rows, norm_rows, delta_part, text_key_rows, text_value_rows, None)
        query_tile = (video_query + text_query).astype(jnp.bfloat16).reshape(tile_shape)
        window_grad = jnp.stack((video_key, video_value)).reshape((2,) + window_shape)
        start = (anchor, anchor, row_start, col_start, anchor)
        current = lax.dynamic_slice(grad_pad, start, window_grad.shape)
        grad_pad = lax.dynamic_update_slice(grad_pad, current + window_grad, start)
        text_total = text_total + jnp.stack((text_key, text_value))
        return (grad_pad, text_total), query_tile

    grad_start = jnp.zeros((2, frames, rows_all + 2 * halo_rim, cols_all + 2 * halo_rim, width), jnp.float32)
    text_start = jnp.zeros((2, TEXT, HEADS, HDIM), jnp.float32)
    (grad_pad, text_total), query_tiles = lax.scan(per_tile, (grad_start, text_start), jnp.arange(N_HA * N_WA, dtype=jnp.int32))
    folded = grad_pad[:, :, halo_rim:halo_rim + rows_all]
    folded = folded.at[:, :, :halo_rim].add(grad_pad[:, :, halo_rim + rows_all:])
    folded = folded.at[:, :, rows_all - halo_rim:].add(grad_pad[:, :, :halo_rim])
    core = folded[:, :, :, halo_rim:halo_rim + cols_all]
    core = core.at[:, :, :, :halo_rim].add(folded[:, :, :, halo_rim + cols_all:])
    core = core.at[:, :, :, cols_all - halo_rim:].add(folded[:, :, :, :halo_rim])
    query_grad = query_tiles.reshape(N_HA, N_WA, frames, tile_side, tile_side, width)
    query_grad = query_grad.transpose(2, 0, 3, 1, 4, 5).reshape(frames, rows_all, cols_all, width)
    text_key_grad = text_total[0].reshape(TEXT, HEADS * HDIM).astype(jnp.bfloat16)
    text_value_grad = text_total[1].reshape(TEXT, HEADS * HDIM).astype(jnp.bfloat16)
    return query_grad, core[0].astype(jnp.bfloat16), core[1].astype(jnp.bfloat16), text_key_grad, text_value_grad
```

```python
import functools
import math

import jax
import jax.numpy as jnp
import numpy as np
from jax import lax
from jax.experimental import pallas as pl
from jax.experimental.pallas import tpu as pltpu
from jax.sharding import PartitionSpec as P

HEADS = 12
HDIM = 128
TILE = 8
HALO = 2
FRAMES = 2
WIDTH = HEADS * HDIM
CELLS = FRAMES * TILE * TILE
TEXT = 32
CHUNKS = 3
PER_CHUNK = HEADS // CHUNKS
LANES = PER_CHUNK * HDIM
TILES = HEADS * TEXT // 8
SCALE = 1.0 / math.sqrt(HDIM)

TOP, RIGHT, BOTTOM, LEFT, LAST = 4, 7, 10, 13, 16
UP, UP_LEFT, UP_RIGHT, DOWN, DOWN_LEFT, DOWN_RIGHT, WEST, EAST, BORROWED = 0, 4, 5, 6, 10, 11, 12, 16, 20

F32 = jnp.float32
BF16 = jnp.bfloat16
NT = (((1,), (1,)), ((), ()))
NN = (((1,), (0,)), ((), ()))
TN = (((0,), (0,)), ((), ()))


def dot(left, right, dims, precision=None):
    return lax.dot_general(left, right, dims, precision=precision, preferred_element_type=F32)


def region_rows():
    low, mid, high = range(0, HALO), range(HALO, TILE - HALO), range(TILE - HALO, TILE)
    regions = (
        (mid, mid), (low, low), (low, mid), (low, high), (mid, high),
        (high, high), (high, mid), (high, low), (mid, low), (low, low),
    )
    return [
        (frame * TILE + row) * TILE + col
        for rows, cols in regions
        for frame in range(FRAMES)
        for row in rows
        for col in cols
    ]


def tile_grads(key, value, query, cotangent, norm, delta, mask):
    scores = dot(key, query, NT) * SCALE
    probs = jnp.exp(scores - norm)
    if mask is not None:
        probs = probs * mask
    prob_grad = dot(value, cotangent, NT)
    score_grad = (probs * (prob_grad - delta)).astype(BF16)
    value_part = dot(probs.astype(BF16), cotangent, NN)
    key_part = dot(score_grad, query, NN)
    query_part = dot(score_grad, key, TN)
    return query_part, key_part, value_part


def kernel(
    n_ha, n_wa,
    q_hbm, k_hbm, v_hbm, o_hbm, norm_hbm, delta_hbm, tk_hbm, tv_hbm, table, order_hbm, back_hbm,
    dq_out, dk_out, dv_out, text_out,
    q, k, v, o, norm4, delta4, tk, tv, order, back,
    norm, delta, mask, packed, own, halo, rim, rows_in, cols_in, acc, dq,
    tpart, tsib, tchip, xin, zpart, zin, zdup, zall, tfin,
    load_sem, halo_send, halo_recv, rows_send, rows_recv, cols_send, cols_recv,
    pair_send, pair_recv, x_send, x_recv, z_send, z_recv, za_send, za_recv, xa_send, xa_recv,
):
    n_x = n_ha // 2
    owned = TILES // n_x
    ha, wa = lax.axis_index("ha"), lax.axis_index("wa")
    x, core = ha // 2, ha % 2
    up, down = (ha + n_ha - 1) % n_ha, (ha + 1) % n_ha
    left, right = (wa + n_wa - 1) % n_wa, (wa + 1) % n_wa
    sibling = 2 * x + 1 - core

    def remote(src, dst, send, recv, **where):
        return pltpu.make_async_remote_copy(
            src_ref=src, dst_ref=dst, send_sem=send, recv_sem=recv,
            device_id=where, device_id_type=pl.DeviceIdType.MESH,
        )

    def wait_bytes(ref, sem):
        pltpu.make_async_copy(ref, ref, sem).wait()

    barrier = pltpu.get_barrier_semaphore()
    greeted = [{"ha": (ha + 2 * step) % n_ha} for step in range(1, n_x)]
    greeted += [{"ha": up}, {"ha": down}]
    greeted += [{"ha": row, "wa": col} for row in (up, down) for col in (left, right)]
    greeted += [{"wa": left}, {"wa": right}]
    for where in greeted:
        pl.semaphore_signal(barrier, inc=1, device_id=where, device_id_type=pl.DeviceIdType.MESH)

    @pl.when(wa == 0)
    def _():
        for col in range(1, n_wa):
            pl.semaphore_signal(barrier, inc=1, device_id={"wa": col}, device_id_type=pl.DeviceIdType.MESH)

    loads = [
        pltpu.make_async_copy(src, dst, load_sem.at[at])
        for at, (src, dst) in enumerate((
            (norm_hbm, norm4), (delta_hbm, delta4), (tk_hbm, tk), (tv_hbm, tv), (q_hbm, q), (o_hbm, o),
            (order_hbm, order), (k_hbm, k), (v_hbm, v), (back_hbm, back),
        ))
    ]
    for load in loads:
        load.start()

    for load, src, dst in ((loads[0], norm4, norm), (loads[1], delta4, delta)):
        load.wait()
        dst[0:HEADS, :] = src[...].T

    for load in loads[2:6]:
        load.wait()
    for head in range(HEADS):
        at = pl.ds(head * HDIM, HDIM)
        query_part, key_part, value_part = tile_grads(
            tk[:, at], tv[:, at], q[:, at], o[:, at], norm[head:head + 1, :], delta[head:head + 1, :], None
        )
        dq[:, at] = query_part
        tpart[0, 4 * head:4 * head + 4] = (key_part * SCALE).reshape(4, 8, HDIM)
        tpart[1, 4 * head:4 * head + 4] = value_part.reshape(4, 8, HDIM)

    for load in loads[6:10]:
        load.wait()
    for at, src in ((0, k), (1, v)):
        for chunk in range(CHUNKS):
            lanes = pl.ds(chunk * LANES, LANES)
            moved = dot(order[...], src[:, lanes], NN)
            packed[at, :, :, lanes] = moved.reshape(LAST + 1, 8, LANES).astype(BF16)
            own[at, :, lanes] = moved[0:CELLS].astype(BF16)

    live = [table[block, ha, wa].astype(F32) for block in range(9)]
    for start, count, block in (
        (UP, 4, 1), (UP_LEFT, 1, 0), (UP_RIGHT, 1, 2), (DOWN, 4, 7), (DOWN_LEFT, 1, 6), (DOWN_RIGHT, 1, 8),
        (WEST, 4, 3), (EAST, 4, 5),
    ):
        mask[8 * start:8 * (start + count), :] = jnp.full((8 * count, CELLS), live[block], F32)

    pl.semaphore_wait(barrier, len(greeted) + jnp.where(wa == 0, 0, 1))

    pair = remote(tpart.at[1 - core], tsib, pair_send.at[0], pair_recv.at[0], ha=sibling)
    pair.start()

    def send_halo(chunk):
        lanes = pl.ds(chunk * LANES, LANES)
        for src, dst, count, where in (
            (LEFT, EAST, 4, {"wa": left}),
            (RIGHT, WEST, 4, {"wa": right}),
            (TOP, DOWN, 4, {"ha": up}),
            (BOTTOM, UP, 4, {"ha": down}),
            (TOP, DOWN_RIGHT, 1, {"ha": up, "wa": left}),
            (RIGHT, DOWN_LEFT, 1, {"ha": up, "wa": right}),
            (LEFT, UP_RIGHT, 1, {"ha": down, "wa": left}),
            (BOTTOM, UP_LEFT, 1, {"ha": down, "wa": right}),
        ):
            remote(
                packed.at[:, src:src + count, :, lanes], halo.at[:, dst:dst + count, :, lanes],
                halo_send.at[chunk], halo_recv.at[chunk], **where,
            ).start()

    send_halo(0)

    pair.wait()
    tchip[...] = (tpart[core] + tsib[...]).reshape(n_x, owned, 8, HDIM)
    for step in range(1, n_x):
        to = (x + step) % n_x
        remote(tchip.at[to], xin.at[step - 1], x_send.at[0], x_recv.at[0], ha=2 * to + core).start()

    for chunk in range(1, CHUNKS):
        send_halo(chunk)

    for head in range(HEADS):
        at = pl.ds(head * HDIM, HDIM)
        query_part, key_part, value_part = tile_grads(
            own[0, :, at], own[1, :, at], q[:, at], o[:, at],
            norm[head:head + 1, :], delta[head:head + 1, :], live[4],
        )
        dq[:, at] += query_part
        acc[0, :, :, at] = key_part.reshape(CELLS // 8, 8, HDIM)
        acc[1, :, :, at] = value_part.reshape(CELLS // 8, 8, HDIM)

    def rim_grads(chunk):
        lanes = pl.ds(chunk * LANES, LANES)
        wait_bytes(halo.at[:, :, :, lanes], halo_recv.at[chunk])
        for head in range(chunk * PER_CHUNK, (chunk + 1) * PER_CHUNK):
            at = pl.ds(head * HDIM, HDIM)
            query_part, key_part, value_part = tile_grads(
                halo[0, :, :, at].reshape(8 * BORROWED, HDIM), halo[1, :, :, at].reshape(8 * BORROWED, HDIM),
                q[:, at], o[:, at], norm[head:head + 1, :], delta[head:head + 1, :], mask[...],
            )
            dq[:, at] += query_part
            rim[0, :, :, at] = key_part.reshape(BORROWED, 8, HDIM)
            rim[1, :, :, at] = value_part.reshape(BORROWED, 8, HDIM)
        for side, start, where in ((0, UP, up), (1, DOWN, down)):
            remote(
                rim.at[:, start:start + 6, :, lanes], rows_in.at[side, :, :, :, lanes],
                rows_send.at[side, chunk], rows_recv.at[side, chunk], ha=where,
            ).start()

    def cols_out(chunk):
        lanes = pl.ds(chunk * LANES, LANES)
        for side in range(2):
            wait_bytes(rows_in.at[side, :, :, :, lanes], rows_recv.at[side, chunk])
        rim[:, WEST, :, lanes] += rows_in[1, :, 4, :, lanes]
        rim[:, WEST + 3, :, lanes] += rows_in[0, :, 4, :, lanes]
        rim[:, EAST, :, lanes] += rows_in[0, :, 5, :, lanes]
        rim[:, EAST + 3, :, lanes] += rows_in[1, :, 5, :, lanes]
        for side, start, where in ((0, WEST, left), (1, EAST, right)):
            remote(
                rim.at[:, start:start + 4, :, lanes], cols_in.at[side, :, :, :, lanes],
                cols_send.at[side, chunk], cols_recv.at[side, chunk], wa=where,
            ).start()

    def finish(chunk):
        lanes = pl.ds(chunk * LANES, LANES)
        acc[:, BOTTOM:BOTTOM + 4, :, lanes] += rows_in[0, :, 0:4, :, lanes]
        acc[:, TOP:TOP + 4, :, lanes] += rows_in[1, :, 0:4, :, lanes]
        for side in range(2):
            wait_bytes(cols_in.at[side, :, :, :, lanes], cols_recv.at[side, chunk])
        acc[:, RIGHT:RIGHT + 4, :, lanes] += cols_in[0, :, :, :, lanes]
        acc[:, LEFT:LEFT + 3, :, lanes] += cols_in[1, :, 0:3, :, lanes]
        acc[:, TOP, :, lanes] += cols_in[1, :, 3, :, lanes]
        for at, out, factor in ((0, dk_out, SCALE), (1, dv_out, 1.0)):
            total = (acc[at, :, :, lanes] * factor).reshape(CELLS, LANES).astype(BF16)
            out[:, lanes] = dot(back[...], total, NN).astype(BF16)

    def gather_x():
        tfin[core, x] = zall[...]
        for step in range(1, n_x):
            to = (x + step) % n_x
            remote(zall, tfin.at[core, x], xa_send.at[0], xa_recv.at[0], ha=2 * to + core).start()

    rim_grads(0)
    rim_grads(1)

    wait_bytes(xin, x_recv.at[0])
    total = tchip[x]
    for step in range(n_x - 1):
        total = total + xin[step]
    zpart[...] = total

    @pl.when(wa != 0)
    def _():
        remote(zpart, zin.at[wa - 1], z_send.at[0], z_recv.at[0], wa=0).start()

    rim_grads(2)
    cols_out(0)
    cols_out(1)

    @pl.when(wa == 0)
    def _():
        wait_bytes(zin, z_recv.at[0])
        final = zpart[...]
        for col in range(n_wa - 1):
            final = final + zin[col]
        final = final.astype(BF16)
        zall[...] = final
        gather_x()
        for col in range(1, n_wa):
            remote(zall, zall, za_send.at[0], za_recv.at[0], wa=col).start()

    cols_out(2)
    dq_out[...] = (dq[...] * SCALE).astype(BF16)
    finish(0)
    finish(1)

    @pl.when(wa != 0)
    def _():
        wait_bytes(zall, za_recv.at[0])
        gather_x()

    finish(2)

    wait_bytes(tfin.at[core, 0:n_x - 1], xa_recv.at[0])
    pair = remote(tfin.at[core], tfin.at[core], pair_send.at[1], pair_recv.at[1], ha=sibling)
    pair.start()
    wait_bytes(tfin.at[1 - core], pair_recv.at[1])
    for at in range(2):
        for tile in range(TILES):
            text_out[at, tile % 4, :, (tile // 4) * HDIM:(tile // 4 + 1) * HDIM] = tfin[at, tile // owned, tile % owned]
    pair.wait_send()
    for chunk in range(CHUNKS):
        lanes = pl.ds(chunk * LANES, LANES)
        wait_bytes(halo.at[:, :, :, lanes], halo_send.at[chunk])
        for side in range(2):
            wait_bytes(rows_in.at[side, :, :, :, lanes], rows_send.at[side, chunk])
            wait_bytes(cols_in.at[side, :, :, :, lanes], cols_send.at[side, chunk])
    wait_bytes(xin, x_send.at[0])
    @pl.when(wa != 0)
    def _():
        wait_bytes(zpart, z_send.at[0])

    @pl.when(wa == 0)
    def _():
        wait_bytes(zdup, za_send.at[0])

    wait_bytes(tfin.at[core, 0:n_x - 1], xa_send.at[0])


def store(dq, dk, dv, text, dq_hbm, dk_hbm, dv_hbm, dtk_hbm, dtv_hbm, sem):
    copies = [
        pltpu.make_async_copy(src, dst, sem.at[at])
        for at, (src, dst) in enumerate((
            (dq, dq_hbm), (dk, dk_hbm), (dv, dv_hbm), (text.at[0], dtk_hbm), (text.at[1], dtv_hbm),
        ))
    ]
    for copy in copies:
        copy.start()
    for copy in copies:
        copy.wait()


def local(n_ha, n_wa, queries, keys, values, out_grad, log_norm, delta_rows, text_keys, text_values, window_table):
    n_x = n_ha // 2
    owned = TILES // n_x
    rows = region_rows()
    order = np.zeros((8 * (LAST + 1), CELLS), np.float32)
    order[np.arange(len(rows)), rows] = 1.0
    back = order[:CELLS].T
    hbm = pl.BlockSpec(memory_space=pl.ANY)
    vmem = pltpu.VMEM
    dma = pltpu.SemaphoreType.DMA
    flat = (CELLS, WIDTH)
    outs = pl.pallas_call(
        functools.partial(kernel, n_ha, n_wa),
        out_shape=[vmem(flat, BF16)] * 3 + [vmem((2, TEXT // 8, 8, WIDTH), BF16)],
        in_specs=[hbm] * 8 + [pl.BlockSpec(memory_space=pltpu.SMEM)] + [hbm] * 2,
        out_specs=[pl.BlockSpec(memory_space=vmem)] * 4,
        scratch_shapes=[
            vmem(flat, BF16), vmem(flat, BF16), vmem(flat, BF16), vmem(flat, BF16),
            vmem((CELLS, HEADS), F32), vmem((CELLS, HEADS), F32),
            vmem((TEXT, WIDTH), BF16), vmem((TEXT, WIDTH), BF16),
            vmem((8 * (LAST + 1), CELLS), BF16), vmem((CELLS, CELLS), BF16),
            vmem((16, CELLS), F32), vmem((16, CELLS), F32), vmem((8 * BORROWED, CELLS), F32),
            vmem((2, LAST + 1, 8, WIDTH), BF16), vmem((2, CELLS, WIDTH), BF16),
            vmem((2, BORROWED, 8, WIDTH), BF16), vmem((2, BORROWED, 8, WIDTH), F32),
            vmem((2, 2, 6, 8, WIDTH), F32), vmem((2, 2, 4, 8, WIDTH), F32),
            vmem((2, CELLS // 8, 8, WIDTH), F32), vmem(flat, F32),
            vmem((2, TILES, 8, HDIM), F32), vmem((TILES, 8, HDIM), F32), vmem((n_x, owned, 8, HDIM), F32),
            vmem((n_x - 1, owned, 8, HDIM), F32), vmem((owned, 8, HDIM), F32), vmem((n_wa - 1, owned, 8, HDIM), F32),
            vmem((n_wa - 1, owned, 8, HDIM), BF16), vmem((owned, 8, HDIM), BF16), vmem((2, n_x, owned, 8, HDIM), BF16),
            dma((10,)), dma((CHUNKS,)), dma((CHUNKS,)),
            dma((2, CHUNKS)), dma((2, CHUNKS)), dma((2, CHUNKS)), dma((2, CHUNKS)),
            dma((2,)), dma((2,)), dma((1,)), dma((1,)), dma((1,)), dma((1,)),
            dma((1,)), dma((1,)), dma((1,)), dma((1,)),
        ],
        compiler_params=pltpu.CompilerParams(collective_id=0, has_side_effects=True, vmem_limit_bytes=56 << 20),
    )(
        queries.reshape(flat), keys.reshape(flat), values.reshape(flat), out_grad.reshape(flat),
        log_norm.transpose(1, 2, 3, 0).reshape(CELLS, HEADS), delta_rows.transpose(1, 2, 3, 0).reshape(CELLS, HEADS),
        text_keys, text_values, window_table.transpose(2, 0, 1),
        jnp.asarray(order, BF16), jnp.asarray(back, BF16),
    )
    outs = pl.pallas_call(
        store,
        out_shape=[jax.ShapeDtypeStruct(flat, BF16)] * 3 + [jax.ShapeDtypeStruct((TEXT // 8, 8, WIDTH), BF16)] * 2,
        in_specs=[pl.BlockSpec(memory_space=vmem)] * 4,
        out_specs=[hbm] * 5,
        scratch_shapes=[dma((5,))],
        compiler_params=pltpu.CompilerParams(has_side_effects=True, vmem_limit_bytes=1 << 20),
    )(*outs)
    cells = queries.shape
    return (
        outs[0].reshape(cells), outs[1].reshape(cells), outs[2].reshape(cells),
        outs[3].reshape(TEXT, WIDTH), outs[4].reshape(TEXT, WIDTH),
    )


def solution(mesh):
    cells = P("group", "ha", "wa", None)
    stats = P(None, "group", "ha", "wa")
    text = P("group", None)
    return jax.shard_map(
        functools.partial(local, mesh.shape["ha"], mesh.shape["wa"]),
        mesh=mesh,
        in_specs=(cells, cells, cells, cells, stats, stats, text, text, P()),
        out_specs=(cells, cells, cells, text, text),
        check_vma=False,
    )
```

```python
import functools
import math

import jax
import jax.numpy as jnp
import numpy as np
from jax import lax
from jax.experimental import pallas as pl
from jax.experimental.pallas import tpu as pltpu
from jax.sharding import PartitionSpec as P

HEADS = 12
HDIM = 128
TILE = 8
HALO = 2
FRAMES = 2
WIDTH = HEADS * HDIM
CELLS = FRAMES * TILE * TILE
TEXT = 32
CHUNKS = 3
PER_CHUNK = HEADS // CHUNKS
LANES = PER_CHUNK * HDIM
TILES = HEADS * TEXT // 8
SCALE = 1.0 / math.sqrt(HDIM)

TOP, RIGHT, BOTTOM, LEFT, LAST = 4, 7, 10, 13, 16
EAST, UP_RIGHT, DOWN_RIGHT, UP, DOWN, WEST, UP_LEFT, DOWN_LEFT, BORROWED = 0, 4, 5, 6, 10, 14, 18, 19, 20
PARTS = ((0, 6), (6, 14), (14, 20))

F32 = jnp.float32
BF16 = jnp.bfloat16
NT = (((1,), (1,)), ((), ()))
NN = (((1,), (0,)), ((), ()))
TN = (((0,), (0,)), ((), ()))


def dot(left, right, dims, precision=None):
    return lax.dot_general(left, right, dims, precision=precision, preferred_element_type=F32)


def region_rows():
    low, mid, high = range(0, HALO), range(HALO, TILE - HALO), range(TILE - HALO, TILE)
    regions = (
        (mid, mid), (low, low), (low, mid), (low, high), (mid, high),
        (high, high), (high, mid), (high, low), (mid, low), (low, low),
    )
    return [
        (frame * TILE + row) * TILE + col
        for rows, cols in regions
        for frame in range(FRAMES)
        for row in rows
        for col in cols
    ]


def score_grads(key, value, query, cotangent, norm, delta, mask):
    probs = jnp.exp(dot(key, query, NT) * SCALE - norm)
    if mask is not None:
        probs = probs * mask
    score_grad = (probs * (dot(value, cotangent, NT) - delta)).astype(BF16)
    return probs.astype(BF16), score_grad


def kernel(
    n_ha, n_wa,
    q_hbm, k_hbm, v_hbm, o_hbm, norm_hbm, delta_hbm, tk_hbm, tv_hbm, table_hbm, order_hbm, back_hbm,
    dq_out, dk_out, dv_out, text_out,
    q, k, v, o, norm12, delta12, tk, tv, order, back, table,
    norm, delta, mask, packed, own, halo, rim, rows_in, corner_in, cols_in, acc, dq, text_grad,
    tpart, tsib, tchip, xin, zpart, zin, zall, tfin,
    load_sem, halo_send, halo_recv, rows_send, rows_recv, corner_send, corner_recv, cols_send, cols_recv,
    pair_send, pair_recv, x_send, x_recv, z_send, z_recv, za_send, za_recv, xa_send, xa_recv, ready,
):
    n_x = n_ha // 2
    owned = TILES // n_x
    ha, wa = lax.axis_index("ha"), lax.axis_index("wa")
    x, core = ha // 2, ha % 2
    up, down = (ha + n_ha - 1) % n_ha, (ha + 1) % n_ha
    left, right = (wa + n_wa - 1) % n_wa, (wa + 1) % n_wa
    sibling = 2 * x + 1 - core

    def remote(src, dst, send, recv, **where):
        return pltpu.make_async_remote_copy(
            src_ref=src, dst_ref=dst, send_sem=send, recv_sem=recv,
            device_id=where, device_id_type=pl.DeviceIdType.MESH,
        )

    def signal(sem, **where):
        pl.semaphore_signal(sem, inc=1, device_id=where, device_id_type=pl.DeviceIdType.MESH)

    def wait_bytes(ref, sem):
        pltpu.make_async_copy(ref, ref, sem).wait()

    def lanes_of(chunk):
        return pl.ds(chunk * LANES, LANES)

    barrier = pltpu.get_barrier_semaphore()
    for col in (left,):
        signal(barrier, wa=col)
        signal(barrier, ha=up, wa=col)
        signal(barrier, ha=down, wa=col)
    signal(barrier, ha=up)
    signal(barrier, ha=down)
    for step in range(1, n_x):
        signal(barrier, ha=(ha + 2 * step) % n_ha)

    loads = [
        pltpu.make_async_copy(src, dst, load_sem.at[at])
        for at, (src, dst) in enumerate((
            (k_hbm, k), (v_hbm, v), (order_hbm, order), (norm_hbm, norm12), (delta_hbm, delta12),
            (tk_hbm, tk), (tv_hbm, tv), (q_hbm, q), (o_hbm, o), (table_hbm, table), (back_hbm, back),
        ))
    ]
    for load in loads:
        load.start()

    @pl.when(wa == 0)
    def _():
        for col in range(1, n_wa):
            signal(barrier, wa=col)

    def send_halo(part, chunk, sends):
        lanes = lanes_of(chunk)
        for src, dst, count, where in sends:
            to_part = [at for at, (low, high) in enumerate(PARTS) if low <= dst < high][0]
            remote(
                packed.at[:, src:src + count, :, lanes], halo.at[:, dst:dst + count, :, lanes],
                halo_send.at[part, chunk], halo_recv.at[to_part, chunk], **where,
            ).start()

    def enter():
        pl.semaphore_wait(barrier, 5 + n_x - 1 + jnp.where(wa == 0, 0, 1))
        signal(ready.at[0], wa=right)
        signal(ready.at[1], ha=up, wa=right)
        signal(ready.at[1], ha=down, wa=right)
        for chunk in range(CHUNKS):
            send_halo(0, chunk, (
                (RIGHT, WEST, 4, {"wa": right}),
                (RIGHT, DOWN_LEFT, 1, {"ha": up, "wa": right}),
                (BOTTOM, UP_LEFT, 1, {"ha": down, "wa": right}),
            ))
            send_halo(1, chunk, ((TOP, DOWN, 4, {"ha": up}), (BOTTOM, UP, 4, {"ha": down})))

    def send_west():
        pl.semaphore_wait(ready.at[0], 1)
        for chunk in range(CHUNKS):
            send_halo(2, chunk, ((LEFT, EAST, 4, {"wa": left}),))
        pl.semaphore_wait(ready.at[1], 2)
        for chunk in range(CHUNKS):
            send_halo(2, chunk, (
                (TOP, DOWN_RIGHT, 1, {"ha": up, "wa": left}),
                (LEFT, UP_RIGHT, 1, {"ha": down, "wa": left}),
            ))

    for load in loads[0:3]:
        load.wait()
    for at, src in ((0, k), (1, v)):
        for chunk in range(CHUNKS):
            moved = dot(order[...], src[:, lanes_of(chunk)], NN)
            packed[at, :, :, lanes_of(chunk)] = moved.reshape(LAST + 1, 8, LANES).astype(BF16)
            own[at, :, lanes_of(chunk)] = moved[0:CELLS].astype(BF16)

    late = (wa == n_wa - 1) | ((wa == 0) & (ha == 0))
    pl.when(late)(enter)

    for load, src, dst in ((loads[3], norm12, norm), (loads[4], delta12, delta)):
        load.wait()
        dst[0:HEADS, :] = src[...].T

    def statistics(head):
        return norm[head:head + 1, :], delta[head:head + 1, :]

    for load in loads[5:9]:
        load.wait()
    for head in range(HEADS):
        at = pl.ds(head * HDIM, HDIM)
        probs, score_grad = score_grads(tk[:, at], tv[:, at], q[:, at], o[:, at], *statistics(head), None)
        text_grad[head] = score_grad
        tpart[0, 4 * head:4 * head + 4] = (dot(score_grad, q[:, at], NN) * SCALE).reshape(4, 8, HDIM)
        tpart[1, 4 * head:4 * head + 4] = dot(probs, o[:, at], NN).reshape(4, 8, HDIM)

    pl.when(jnp.logical_not(late))(enter)

    pair = remote(tpart.at[1 - core], tsib, pair_send.at[0], pair_recv.at[0], ha=sibling)
    pair.start()

    pl.when(wa != 0)(send_west)

    for load in loads[9:11]:
        load.wait()
    live = [table[block, ha, wa].astype(F32) for block in range(9)]
    for start, count, block in (
        (UP, 4, 1), (UP_LEFT, 1, 0), (UP_RIGHT, 1, 2), (DOWN, 4, 7), (DOWN_LEFT, 1, 6), (DOWN_RIGHT, 1, 8),
        (WEST, 4, 3), (EAST, 4, 5),
    ):
        mask[8 * start:8 * (start + count), :] = jnp.full((8 * count, CELLS), live[block], F32)

    pair.wait_recv()
    tchip[...] = (tpart[core] + tsib[...]).reshape(n_x, owned, 8, HDIM)
    for step in range(1, n_x):
        to = (x + step) % n_x
        remote(tchip.at[to], xin.at[step - 1], x_send.at[0], x_recv.at[0], ha=2 * to + core).start()

    def rim_grads(part, chunk):
        low, high = PARTS[part]
        rows = 8 * (high - low)
        lanes = lanes_of(chunk)
        wait_bytes(halo.at[:, low:high, :, lanes], halo_recv.at[part, chunk])
        for head in range(chunk * PER_CHUNK, (chunk + 1) * PER_CHUNK):
            at = pl.ds(head * HDIM, HDIM)
            key, value = (halo[kind, low:high, :, at].reshape(rows, HDIM) for kind in range(2))
            probs, score_grad = score_grads(
                key, value, q[:, at], o[:, at], *statistics(head), mask[8 * low:8 * high, :]
            )
            rim[0, low:high, :, at] = dot(score_grad, q[:, at], NN).reshape(high - low, 8, HDIM)
            rim[1, low:high, :, at] = dot(probs, o[:, at], NN).reshape(high - low, 8, HDIM)
            query_part = dot(score_grad, key, TN)
            dq[:, at] = query_part if part == 0 else dq[:, at] + query_part

    def corners_out(side, chunk):
        lanes = lanes_of(chunk)
        for source, start, where in ((0, (UP_RIGHT, UP_LEFT)[side], up), (1, (DOWN_RIGHT, DOWN_LEFT)[side], down)):
            remote(
                rim.at[:, start, :, lanes], corner_in.at[side, source, :, :, lanes],
                corner_send.at[side, chunk], corner_recv.at[side, chunk], ha=where,
            ).start()

    def cols_out(side, chunk):
        lanes = lanes_of(chunk)
        wait_bytes(corner_in.at[side, :, :, :, lanes], corner_recv.at[side, chunk])
        start, where = ((EAST, right), (WEST, left))[side]
        below, above = ((start, start + 3), (start + 3, start))[side]
        rim[:, below, :, lanes] += corner_in[side, 0, :, :, lanes]
        rim[:, above, :, lanes] += corner_in[side, 1, :, :, lanes]
        remote(
            rim.at[:, start:start + 4, :, lanes], cols_in.at[side, :, :, :, lanes],
            cols_send.at[side, chunk], cols_recv.at[side, chunk], wa=where,
        ).start()

    def rows_out(chunk):
        lanes = lanes_of(chunk)
        for source, start, where in ((0, UP, up), (1, DOWN, down)):
            remote(
                rim.at[:, start:start + 4, :, lanes], rows_in.at[source, :, :, :, lanes],
                rows_send.at[chunk], rows_recv.at[chunk], ha=where,
            ).start()

    for chunk in range(CHUNKS):
        rim_grads(0, chunk)
        corners_out(0, chunk)

    pl.when(wa == 0)(send_west)

    for chunk in range(CHUNKS):
        cols_out(0, chunk)
    for chunk in range(CHUNKS):
        rim_grads(1, chunk)
        rows_out(chunk)

    wait_bytes(xin, x_recv.at[0])
    total = tchip[x]
    for step in range(n_x - 1):
        total = total + xin[step]
    zpart[...] = total

    @pl.when(wa != 0)
    def _():
        remote(zpart, zin.at[wa - 1], z_send.at[0], z_recv.at[0], wa=0).start()

    for head in range(HEADS):
        at = pl.ds(head * HDIM, HDIM)
        probs, score_grad = score_grads(own[0, :, at], own[1, :, at], q[:, at], o[:, at], *statistics(head), live[4])
        acc[0, :, :, at] = dot(score_grad, q[:, at], NN).reshape(CELLS // 8, 8, HDIM)
        acc[1, :, :, at] = dot(probs, o[:, at], NN).reshape(CELLS // 8, 8, HDIM)
        dq[:, at] += dot(score_grad, own[0, :, at], TN) + dot(text_grad[head], tk[:, at], TN)

    for chunk in range(CHUNKS):
        rim_grads(2, chunk)
        corners_out(1, chunk)
    for chunk in range(CHUNKS):
        cols_out(1, chunk)

    def gather_x():
        tfin[core, x] = zall[...]
        for step in range(1, n_x):
            to = (x + step) % n_x
            remote(zall, tfin.at[core, x], xa_send.at[0], xa_recv.at[0], ha=2 * to + core).start()

    @pl.when(wa == 0)
    def _():
        wait_bytes(zin, z_recv.at[0])
        final = zpart[...]
        for col in range(n_wa - 1):
            final = final + zin[col]
        zall[...] = final.astype(BF16)
        gather_x()
        for col in range(1, n_wa):
            remote(zall, zall, za_send.at[0], za_recv.at[0], wa=col).start()

    dq_out[...] = (dq[...] * SCALE).astype(BF16)

    @pl.when(wa != 0)
    def _():
        wait_bytes(zall, za_recv.at[0])
        gather_x()

    for chunk in range(CHUNKS):
        lanes = lanes_of(chunk)
        wait_bytes(rows_in.at[:, :, :, :, lanes], rows_recv.at[chunk])
        acc[:, BOTTOM:BOTTOM + 4, :, lanes] += rows_in[0, :, :, :, lanes]
        acc[:, TOP:TOP + 4, :, lanes] += rows_in[1, :, :, :, lanes]
        wait_bytes(cols_in.at[1, :, :, :, lanes], cols_recv.at[1, chunk])
        acc[:, RIGHT:RIGHT + 4, :, lanes] += cols_in[1, :, :, :, lanes]
        wait_bytes(cols_in.at[0, :, :, :, lanes], cols_recv.at[0, chunk])
        acc[:, LEFT:LEFT + 3, :, lanes] += cols_in[0, :, 0:3, :, lanes]
        acc[:, TOP, :, lanes] += cols_in[0, :, 3, :, lanes]
        for at, out, factor in ((0, dk_out, SCALE), (1, dv_out, 1.0)):
            total = (acc[at, :, :, lanes] * factor).reshape(CELLS, LANES).astype(BF16)
            out[:, lanes] = dot(back[...], total, NN).astype(BF16)

    wait_bytes(tfin.at[core, 0:n_x - 1], xa_recv.at[0])
    last = remote(tfin.at[core], tfin.at[core], pair_send.at[1], pair_recv.at[1], ha=sibling)
    last.start()
    wait_bytes(tfin.at[1 - core], pair_recv.at[1])
    for at in range(2):
        for tile in range(TILES):
            text_out[at, tile % 4, :, (tile // 4) * HDIM:(tile // 4 + 1) * HDIM] = tfin[at, tile // owned, tile % owned]

    last.wait_send()
    pair.wait_send()
    for chunk in range(CHUNKS):
        lanes = lanes_of(chunk)
        for part, (low, high) in enumerate(PARTS):
            wait_bytes(halo.at[:, low:high, :, lanes], halo_send.at[part, chunk])
        wait_bytes(rows_in.at[:, :, :, :, lanes], rows_send.at[chunk])
        for side in range(2):
            wait_bytes(corner_in.at[side, :, :, :, lanes], corner_send.at[side, chunk])
            wait_bytes(cols_in.at[side, :, :, :, lanes], cols_send.at[side, chunk])
    wait_bytes(xin, x_send.at[0])

    @pl.when(wa != 0)
    def _():
        wait_bytes(zpart, z_send.at[0])

    @pl.when(wa == 0)
    def _():
        wait_bytes(zin.at[:, :, 0:4, :], za_send.at[0])

    wait_bytes(tfin.at[core, 0:n_x - 1], xa_send.at[0])


def store(dq, dk, dv, text, dq_hbm, dk_hbm, dv_hbm, dtk_hbm, dtv_hbm, sem):
    copies = [
        pltpu.make_async_copy(src, dst, sem.at[at])
        for at, (src, dst) in enumerate((
            (dq, dq_hbm), (dk, dk_hbm), (dv, dv_hbm), (text.at[0], dtk_hbm), (text.at[1], dtv_hbm),
        ))
    ]
    for copy in copies:
        copy.start()
    for copy in copies:
        copy.wait()


def local(n_ha, n_wa, queries, keys, values, out_grad, log_norm, delta_rows, text_keys, text_values, window_table):
    n_x = n_ha // 2
    owned = TILES // n_x
    rows = region_rows()
    order = np.zeros((8 * (LAST + 1), CELLS), np.float32)
    order[np.arange(len(rows)), rows] = 1.0
    back = order[:CELLS].T
    hbm = pl.BlockSpec(memory_space=pl.ANY)
    vmem = pltpu.VMEM
    dma = pltpu.SemaphoreType.DMA
    flat = (CELLS, WIDTH)
    outs = pl.pallas_call(
        functools.partial(kernel, n_ha, n_wa),
        out_shape=[vmem(flat, BF16)] * 3 + [vmem((2, TEXT // 8, 8, WIDTH), BF16)],
        in_specs=[hbm] * 11,
        out_specs=[pl.BlockSpec(memory_space=vmem)] * 4,
        scratch_shapes=[
            vmem(flat, BF16), vmem(flat, BF16), vmem(flat, BF16), vmem(flat, BF16),
            vmem((CELLS, HEADS), F32), vmem((CELLS, HEADS), F32),
            vmem((TEXT, WIDTH), BF16), vmem((TEXT, WIDTH), BF16),
            vmem((8 * (LAST + 1), CELLS), BF16), vmem((CELLS, CELLS), BF16),
            pltpu.SMEM((window_table.shape[2],) + window_table.shape[:2], jnp.int32),
            vmem((16, CELLS), F32), vmem((16, CELLS), F32), vmem((8 * BORROWED, CELLS), F32),
            vmem((2, LAST + 1, 8, WIDTH), BF16), vmem((2, CELLS, WIDTH), BF16),
            vmem((2, BORROWED, 8, WIDTH), BF16), vmem((2, BORROWED, 8, WIDTH), F32),
            vmem((2, 2, 4, 8, WIDTH), F32), vmem((2, 2, 2, 8, WIDTH), F32), vmem((2, 2, 4, 8, WIDTH), F32),
            vmem((2, CELLS // 8, 8, WIDTH), F32), vmem(flat, F32), vmem((HEADS, TEXT, CELLS), BF16),
            vmem((2, TILES, 8, HDIM), F32), vmem((TILES, 8, HDIM), F32), vmem((n_x, owned, 8, HDIM), F32),
            vmem((n_x - 1, owned, 8, HDIM), F32), vmem((owned, 8, HDIM), F32), vmem((n_wa - 1, owned, 8, HDIM), F32),
            vmem((owned, 8, HDIM), BF16), vmem((2, n_x, owned, 8, HDIM), BF16),
            dma((11,)), dma((3, CHUNKS)), dma((3, CHUNKS)), dma((CHUNKS,)), dma((CHUNKS,)),
            dma((2, CHUNKS)), dma((2, CHUNKS)), dma((2, CHUNKS)), dma((2, CHUNKS)),
            dma((2,)), dma((2,)), dma((1,)), dma((1,)), dma((1,)), dma((1,)),
            dma((1,)), dma((1,)), dma((1,)), dma((1,)), pltpu.SemaphoreType.REGULAR((2,)),
        ],
        compiler_params=pltpu.CompilerParams(collective_id=0, has_side_effects=True, vmem_limit_bytes=56 << 20),
    )(
        queries.reshape(flat), keys.reshape(flat), values.reshape(flat), out_grad.reshape(flat),
        log_norm.transpose(1, 2, 3, 0).reshape(CELLS, HEADS), delta_rows.transpose(1, 2, 3, 0).reshape(CELLS, HEADS),
        text_keys, text_values, window_table.transpose(2, 0, 1),
        jnp.asarray(order, BF16), jnp.asarray(back, BF16),
    )
    outs = pl.pallas_call(
        store,
        out_shape=[jax.ShapeDtypeStruct(flat, BF16)] * 3 + [jax.ShapeDtypeStruct((TEXT // 8, 8, WIDTH), BF16)] * 2,
        in_specs=[pl.BlockSpec(memory_space=vmem)] * 4,
        out_specs=[hbm] * 5,
        scratch_shapes=[dma((5,))],
        compiler_params=pltpu.CompilerParams(has_side_effects=True, vmem_limit_bytes=1 << 20),
    )(*outs)
    cells = queries.shape
    return (
        outs[0].reshape(cells), outs[1].reshape(cells), outs[2].reshape(cells),
        outs[3].reshape(TEXT, WIDTH), outs[4].reshape(TEXT, WIDTH),
    )


def solution(mesh):
    cells = P("group", "ha", "wa", None)
    stats = P(None, "group", "ha", "wa")
    text = P("group", None)
    return jax.shard_map(
        functools.partial(local, mesh.shape["ha"], mesh.shape["wa"]),
        mesh=mesh,
        in_specs=(cells, cells, cells, cells, stats, stats, text, text, P()),
        out_specs=(cells, cells, cells, text, text),
        check_vma=False,
    )
```

```python
import functools
import math

import jax
import jax.numpy as jnp
import numpy as np
from jax import lax
from jax.experimental import pallas as pl
from jax.experimental.pallas import tpu as pltpu
from jax.sharding import PartitionSpec as P

HEADS = 12
HDIM = 128
TILE = 8
HALO = 2
FRAMES = 2
WIDTH = HEADS * HDIM
CELLS = FRAMES * TILE * TILE
TEXT = 32
CHUNKS = 3
PER_CHUNK = HEADS // CHUNKS
LANES = PER_CHUNK * HDIM
TILES = HEADS * TEXT // 8
SCALE = 1.0 / math.sqrt(HDIM)

TOP, RIGHT, BOTTOM, LEFT, LAST = 4, 7, 10, 13, 16
EAST, UP_RIGHT, DOWN_RIGHT, UP, DOWN, WEST, UP_LEFT, DOWN_LEFT, BORROWED = 0, 4, 5, 6, 10, 14, 18, 19, 20
PARTS = ((0, 6), (6, 14), (14, 20))

F32 = jnp.float32
BF16 = jnp.bfloat16
NT = (((1,), (1,)), ((), ()))
NN = (((1,), (0,)), ((), ()))
TN = (((0,), (0,)), ((), ()))


def dot(left, right, dims, precision=None):
    return lax.dot_general(left, right, dims, precision=precision, preferred_element_type=F32)


def region_rows():
    low, mid, high = range(0, HALO), range(HALO, TILE - HALO), range(TILE - HALO, TILE)
    regions = (
        (mid, mid), (low, low), (low, mid), (low, high), (mid, high),
        (high, high), (high, mid), (high, low), (mid, low), (low, low),
    )
    return [
        (frame * TILE + row) * TILE + col
        for rows, cols in regions
        for frame in range(FRAMES)
        for row in rows
        for col in cols
    ]


def score_grads(key, value, query, cotangent, norm, delta, mask):
    probs = jnp.exp(dot(key, query, NT) * SCALE - norm)
    if mask is not None:
        probs = probs * mask
    score_grad = (probs * (dot(value, cotangent, NT) - delta)).astype(BF16)
    return probs.astype(BF16), score_grad


def kernel(
    n_ha, n_wa,
    q_hbm, k_hbm, v_hbm, o_hbm, norm_hbm, delta_hbm, tk_hbm, tv_hbm, table_hbm, order_hbm, back_hbm,
    dq_out, dk_out, dv_out, text_out,
    q, k, v, o, norm12, delta12, tk, tv, order, back, table,
    norm, delta, mask, packed, own, halo, rim, rows_in, corner_in, cols_in, acc, grads,
    tpart, tsib, tchip, xin, zpart, zin, zall, tfin,
    load_sem, halo_send, halo_recv, rows_send, rows_recv, corner_send, corner_recv, cols_send, cols_recv,
    pair_send, pair_recv, x_send, x_recv, z_send, z_recv, za_send, za_recv, xa_send, xa_recv, ready, met,
):
    n_x = n_ha // 2
    owned = TILES // n_x
    ha, wa = lax.axis_index("ha"), lax.axis_index("wa")
    x, core = ha // 2, ha % 2
    up, down = (ha + n_ha - 1) % n_ha, (ha + 1) % n_ha
    left, right = (wa + n_wa - 1) % n_wa, (wa + 1) % n_wa
    sibling = 2 * x + 1 - core
    distances = [2 ** at for at in range((n_ha // 4).bit_length())]
    far_first = sorted(range(1, n_x), key=lambda step: -min(step, n_x - step))
    half, helper = n_wa // 2, n_wa // 4 + 1
    corner_device = (wa == 0) & (ha == 0)
    first_owner = (wa == 0) & (ha != 0)
    is_owner = first_owner | (wa == 1)
    greeters = jnp.where(ha == 0, 1, 2) - jnp.where(is_owner, 1, 0)

    def remote(src, dst, send, recv, **where):
        return pltpu.make_async_remote_copy(
            src_ref=src, dst_ref=dst, send_sem=send, recv_sem=recv,
            device_id=where, device_id_type=pl.DeviceIdType.MESH,
        )

    def signal(sem, **where):
        pl.semaphore_signal(sem, inc=1, device_id=where, device_id_type=pl.DeviceIdType.MESH)

    def wait_bytes(ref, sem):
        pltpu.make_async_copy(ref, ref, sem).wait()

    def lanes_of(chunk):
        return pl.ds(chunk * LANES, LANES)

    barrier = pltpu.get_barrier_semaphore()
    for col in (left,):
        signal(barrier, wa=col)
        signal(barrier, ha=up, wa=col)
        signal(barrier, ha=down, wa=col)
    signal(barrier, ha=up)
    signal(barrier, ha=down)

    @pl.when(wa != 0)
    def _():
        for step in range(1, n_x):
            signal(barrier, ha=(ha + 2 * step) % n_ha)

    loads = [
        pltpu.make_async_copy(src, dst, load_sem.at[at])
        for at, (src, dst) in enumerate((
            (k_hbm, k), (v_hbm, v), (order_hbm, order), (norm_hbm, norm12), (delta_hbm, delta12),
            (tk_hbm, tk), (tv_hbm, tv), (q_hbm, q), (o_hbm, o), (table_hbm, table), (back_hbm, back),
        ))
    ]
    for load in loads:
        load.start()

    for owner, cond in ((0, first_owner), (1, wa == 1)):

        @pl.when(cond)
        def _():
            for col in range(n_wa):
                if col != owner:
                    signal(barrier, wa=col)

    def send_halo(part, chunk, sends):
        lanes = lanes_of(chunk)
        for src, dst, count, where in sends:
            to_part = [at for at, (low, high) in enumerate(PARTS) if low <= dst < high][0]
            remote(
                packed.at[:, src:src + count, :, lanes], halo.at[:, dst:dst + count, :, lanes],
                halo_send.at[part, chunk], halo_recv.at[to_part, chunk], **where,
            ).start()

    def enter():
        pl.semaphore_wait(barrier, 5 + greeters + jnp.where(wa == 0, 0, n_x - 1))

        @pl.when(wa == 0)
        def _():
            signal(met.at[0], ha=up)
            signal(met.at[0], ha=down)

        signal(ready.at[0], wa=right)
        signal(ready.at[1], ha=up, wa=right)
        signal(ready.at[1], ha=down, wa=right)
        for chunk in range(CHUNKS):
            send_halo(0, chunk, (
                (RIGHT, WEST, 4, {"wa": right}),
                (RIGHT, DOWN_LEFT, 1, {"ha": up, "wa": right}),
                (BOTTOM, UP_LEFT, 1, {"ha": down, "wa": right}),
            ))

    def meet_row(at):
        pl.semaphore_wait(met.at[at], 2)
        if at + 1 < len(distances):
            signal(met.at[at + 1], ha=(ha + distances[at + 1]) % n_ha)
            signal(met.at[at + 1], ha=(ha + n_ha - distances[at + 1]) % n_ha)

    def send_rows():
        for chunk in range(CHUNKS):
            send_halo(1, chunk, ((TOP, DOWN, 4, {"ha": up}), (BOTTOM, UP, 4, {"ha": down})))

    def send_west(together):
        side = ((LEFT, EAST, 4, {"wa": left}),)
        corners = (
            (TOP, DOWN_RIGHT, 1, {"ha": up, "wa": left}),
            (LEFT, UP_RIGHT, 1, {"ha": down, "wa": left}),
        )
        pl.semaphore_wait(ready.at[0], 1)
        if together:
            pl.semaphore_wait(ready.at[1], 2)
        for chunk in range(CHUNKS):
            send_halo(2, chunk, side + corners if together else side)
        if not together:
            pl.semaphore_wait(ready.at[1], 2)
            for chunk in range(CHUNKS):
                send_halo(2, chunk, corners)

    for load in loads[0:3]:
        load.wait()
    for at, src in ((0, k), (1, v)):
        for chunk in range(CHUNKS):
            moved = dot(order[...], src[:, lanes_of(chunk)], NN)
            packed[at, :, :, lanes_of(chunk)] = moved.reshape(LAST + 1, 8, LANES).astype(BF16)
            own[at, :, lanes_of(chunk)] = moved[0:CELLS].astype(BF16)

    late = (wa == n_wa - 1) | corner_device
    pl.when(late)(enter)

    for load, src, dst in ((loads[3], norm12, norm), (loads[4], delta12, delta)):
        load.wait()
        dst[0:HEADS, :] = src[...].T

    def statistics(head):
        return norm[head:head + 1, :], delta[head:head + 1, :]

    for load in loads[5:9]:
        load.wait()
    for head in range(HEADS):
        at = pl.ds(head * HDIM, HDIM)
        probs, score_grad = score_grads(tk[:, at], tv[:, at], q[:, at], o[:, at], *statistics(head), None)
        grads[head, 0:TEXT] = score_grad
        tpart[0, 4 * head:4 * head + 4] = (dot(score_grad, q[:, at], NN) * SCALE).reshape(4, 8, HDIM)
        tpart[1, 4 * head:4 * head + 4] = dot(probs, o[:, at], NN).reshape(4, 8, HDIM)

    for load in loads[9:11]:
        load.wait()
    live = [table[block, ha, wa].astype(F32) for block in range(9)]
    for start, count, block in (
        (UP, 4, 1), (UP_LEFT, 1, 0), (UP_RIGHT, 1, 2), (DOWN, 4, 7), (DOWN_LEFT, 1, 6), (DOWN_RIGHT, 1, 8),
        (WEST, 4, 3), (EAST, 4, 5),
    ):
        mask[8 * start:8 * (start + count), :] = jnp.full((8 * count, CELLS), live[block], F32)

    def own_grads():
        for head in range(HEADS):
            at = pl.ds(head * HDIM, HDIM)
            probs, score_grad = score_grads(own[0, :, at], own[1, :, at], q[:, at], o[:, at], *statistics(head), live[4])
            acc[0, :, :, at] = dot(score_grad, q[:, at], NN).reshape(CELLS // 8, 8, HDIM)
            acc[1, :, :, at] = dot(probs, o[:, at], NN).reshape(CELLS // 8, 8, HDIM)
            grads[head, TEXT:TEXT + CELLS] = score_grad

    @pl.when(jnp.logical_not(late))
    def _():
        own_grads()
        enter()

    pair = remote(tpart.at[1 - core], tsib, pair_send.at[0], pair_recv.at[0], ha=sibling)
    pair.start()

    pl.when(jnp.logical_not(late))(send_rows)
    pl.when((wa >= 2) & (wa != n_wa - 1))(lambda: send_west(False))

    @pl.when(wa == 0)
    def _():
        for at in range(len(distances) - 1):
            meet_row(at)
        pl.when(first_owner)(lambda: send_west(True))
        meet_row(len(distances) - 1)

    pair.wait_recv()
    tchip[...] = (tpart[core] + tsib[...]).reshape(n_x, owned, 8, HDIM)
    for step in far_first:
        to = (x + step) % n_x
        remote(tchip.at[to], xin.at[step - 1], x_send.at[0], x_recv.at[0], ha=2 * to + core).start()

    @pl.when(corner_device)
    def _():
        send_rows()
        send_west(True)

    def rim_grads(part, chunk):
        low, high = PARTS[part]
        rows = 8 * (high - low)
        lanes = lanes_of(chunk)
        wait_bytes(halo.at[:, low:high, :, lanes], halo_recv.at[part, chunk])
        for head in range(chunk * PER_CHUNK, (chunk + 1) * PER_CHUNK):
            at = pl.ds(head * HDIM, HDIM)
            key, value = (halo[kind, low:high, :, at].reshape(rows, HDIM) for kind in range(2))
            probs, score_grad = score_grads(
                key, value, q[:, at], o[:, at], *statistics(head), mask[8 * low:8 * high, :]
            )
            rim[0, low:high, :, at] = dot(score_grad, q[:, at], NN).reshape(high - low, 8, HDIM)
            rim[1, low:high, :, at] = dot(probs, o[:, at], NN).reshape(high - low, 8, HDIM)
            grads[head, TEXT + CELLS + 8 * low:TEXT + CELLS + 8 * high] = score_grad

    def corners_out(side, chunk):
        lanes = lanes_of(chunk)
        for source, start, where in ((0, (UP_RIGHT, UP_LEFT)[side], up), (1, (DOWN_RIGHT, DOWN_LEFT)[side], down)):
            remote(
                rim.at[:, start, :, lanes], corner_in.at[side, source, :, :, lanes],
                corner_send.at[side, chunk], corner_recv.at[side, chunk], ha=where,
            ).start()

    def cols_out(side, chunk):
        lanes = lanes_of(chunk)
        wait_bytes(corner_in.at[side, :, :, :, lanes], corner_recv.at[side, chunk])
        start, where = ((EAST, right), (WEST, left))[side]
        below, above = ((start, start + 3), (start + 3, start))[side]
        rim[:, below, :, lanes] += corner_in[side, 0, :, :, lanes]
        rim[:, above, :, lanes] += corner_in[side, 1, :, :, lanes]
        remote(
            rim.at[:, start:start + 4, :, lanes], cols_in.at[side, :, :, :, lanes],
            cols_send.at[side, chunk], cols_recv.at[side, chunk], wa=where,
        ).start()

    def rows_out(chunk):
        lanes = lanes_of(chunk)
        for source, start, where in ((0, UP, up), (1, DOWN, down)):
            remote(
                rim.at[:, start:start + 4, :, lanes], rows_in.at[source, :, :, :, lanes],
                rows_send.at[chunk], rows_recv.at[chunk], ha=where,
            ).start()

    def sum_x():
        wait_bytes(xin, x_recv.at[0])
        total = tchip[x]
        for step in range(n_x - 1):
            total = total + xin[step]
        zpart[...] = total
        for at, cond in enumerate(((wa != 0) & (ha != 0), wa != 1)):

            @pl.when(cond)
            def _():
                remote(zpart, zin.at[wa], z_send.at[at], z_recv.at[0], wa=at).start()

    pl.when(jnp.logical_not(late) & (wa != 0))(sum_x)

    for chunk in range(CHUNKS):
        if chunk == CHUNKS - 1:

            @pl.when(late)
            def _():
                sum_x()
                cols_out(0, 0)

        rim_grads(0, chunk)
        corners_out(0, chunk)

    def east_cols(start):
        for chunk in range(start, CHUNKS):
            cols_out(0, chunk)

    def west_cols():
        for chunk in range(CHUNKS):
            cols_out(1, chunk)

    pl.when(wa == n_wa - 1)(send_rows)
    pl.when(jnp.logical_not(late | first_owner))(lambda: east_cols(0))

    @pl.when(late)
    def _():
        east_cols(1)
        own_grads()

    pl.when(wa == n_wa - 1)(lambda: send_west(False))

    for chunk in range(CHUNKS):
        rim_grads(1, chunk)
        rows_out(chunk)

    @pl.when(first_owner)
    def _():
        sum_x()
        east_cols(0)

    pl.when(wa == 1)(lambda: send_west(False))

    for chunk in range(CHUNKS):
        rim_grads(2, chunk)
        corners_out(1, chunk)

    west_cols()

    def gather_x():
        tfin[core, x] = zall[...]
        for step in far_first:
            to = (x + step) % n_x
            remote(zall, tfin.at[core, x], xa_send.at[0], xa_recv.at[0], ha=2 * to + core).start()

    @pl.when(is_owner)
    def _():
        zin[wa] = zpart[...]
        wait_bytes(zin.at[0:n_wa - 1], z_recv.at[0])
        final = zin[0]
        for col in range(1, n_wa):
            final = final + zin[col]
        zall[...] = final.astype(BF16)
        gather_x()

    served = (
        (first_owner, range(half + 2, n_wa), 0),
        ((wa == 1) & (ha != 0), range(2, half + 2), 0),
        ((wa == 1) & (ha == 0), range(2, half + 2), n_x),
        ((wa == helper) & (ha == 0), range(half + 2, n_wa), 0),
    )
    for cond, cols, rows in served[:3]:

        @pl.when(cond)
        def _():
            for to in range(rows):
                remote(zall, tfin.at[core, x], za_send.at[0], xa_recv.at[0], ha=2 * to, wa=0).start()
            for col in cols:
                remote(zall, zall, za_send.at[0], za_recv.at[0], wa=col).start()

    @pl.when(wa >= 2)
    def _():
        wait_bytes(zall, za_recv.at[0])
        gather_x()

    @pl.when(served[3][0])
    def _():
        for col in served[3][1]:
            remote(zall, zall, za_send.at[0], za_recv.at[0], wa=col).start()

    for head in range(HEADS):
        at = pl.ds(head * HDIM, HDIM)
        keys = jnp.concatenate((tk[:, at], own[0, :, at], halo[0, :, :, at].reshape(8 * BORROWED, HDIM)), axis=0)
        dq_out[:, at] = (dot(grads[head], keys, TN) * SCALE).astype(BF16)

    for chunk in range(CHUNKS):
        lanes = lanes_of(chunk)
        wait_bytes(rows_in.at[:, :, :, :, lanes], rows_recv.at[chunk])
        acc[:, BOTTOM:BOTTOM + 4, :, lanes] += rows_in[0, :, :, :, lanes]
        acc[:, TOP:TOP + 4, :, lanes] += rows_in[1, :, :, :, lanes]
        wait_bytes(cols_in.at[1, :, :, :, lanes], cols_recv.at[1, chunk])
        acc[:, RIGHT:RIGHT + 4, :, lanes] += cols_in[1, :, :, :, lanes]
        wait_bytes(cols_in.at[0, :, :, :, lanes], cols_recv.at[0, chunk])
        acc[:, LEFT:LEFT + 3, :, lanes] += cols_in[0, :, 0:3, :, lanes]
        acc[:, TOP, :, lanes] += cols_in[0, :, 3, :, lanes]
        for at, out, factor in ((0, dk_out, SCALE), (1, dv_out, 1.0)):
            total = (acc[at, :, :, lanes] * factor).reshape(CELLS, LANES).astype(BF16)
            out[:, lanes] = dot(back[...], total, NN).astype(BF16)

    @pl.when(corner_device)
    def _():
        wait_bytes(tfin.at[core], xa_recv.at[0])

    @pl.when(jnp.logical_not(corner_device))
    def _():
        wait_bytes(tfin.at[core, 0:n_x - 1], xa_recv.at[0])

    last = remote(tfin.at[core], tfin.at[core], pair_send.at[1], pair_recv.at[1], ha=sibling)
    last.start()
    wait_bytes(tfin.at[1 - core], pair_recv.at[1])
    for at in range(2):
        for tile in range(TILES):
            text_out[at, tile % 4, :, (tile // 4) * HDIM:(tile // 4 + 1) * HDIM] = tfin[at, tile // owned, tile % owned]

    last.wait_send()
    pair.wait_send()
    for chunk in range(CHUNKS):
        lanes = lanes_of(chunk)
        for part, (low, high) in enumerate(PARTS):
            wait_bytes(halo.at[:, low:high, :, lanes], halo_send.at[part, chunk])
        wait_bytes(rows_in.at[:, :, :, :, lanes], rows_send.at[chunk])
        for side in range(2):
            wait_bytes(corner_in.at[side, :, :, :, lanes], corner_send.at[side, chunk])
            wait_bytes(cols_in.at[side, :, :, :, lanes], cols_send.at[side, chunk])
    wait_bytes(xin, x_send.at[0])

    for at, cond in enumerate(((wa != 0) & (ha != 0), wa != 1)):

        @pl.when(cond)
        def _():
            wait_bytes(zpart, z_send.at[at])

    for cond, cols, rows in served:

        @pl.when(cond)
        def _():
            wait_bytes(zin.at[0:(len(cols) + rows) // 2], za_send.at[0])

    @pl.when(jnp.logical_not(corner_device))
    def _():
        wait_bytes(tfin.at[core, 0:n_x - 1], xa_send.at[0])


def store(dq, dk, dv, text, dq_hbm, dk_hbm, dv_hbm, dtk_hbm, dtv_hbm, sem):
    copies = [
        pltpu.make_async_copy(src, dst, sem.at[at])
        for at, (src, dst) in enumerate((
            (dq, dq_hbm), (dk, dk_hbm), (dv, dv_hbm), (text.at[0], dtk_hbm), (text.at[1], dtv_hbm),
        ))
    ]
    for copy in copies:
        copy.start()
    for copy in copies:
        copy.wait()


def local(n_ha, n_wa, queries, keys, values, out_grad, log_norm, delta_rows, text_keys, text_values, window_table):
    n_x = n_ha // 2
    owned = TILES // n_x
    rows = region_rows()
    order = np.zeros((8 * (LAST + 1), CELLS), np.float32)
    order[np.arange(len(rows)), rows] = 1.0
    back = order[:CELLS].T
    hbm = pl.BlockSpec(memory_space=pl.ANY)
    vmem = pltpu.VMEM
    dma = pltpu.SemaphoreType.DMA
    flat = (CELLS, WIDTH)
    outs = pl.pallas_call(
        functools.partial(kernel, n_ha, n_wa),
        out_shape=[vmem(flat, BF16)] * 3 + [vmem((2, TEXT // 8, 8, WIDTH), BF16)],
        in_specs=[hbm] * 11,
        out_specs=[pl.BlockSpec(memory_space=vmem)] * 4,
        scratch_shapes=[
            vmem(flat, BF16), vmem(flat, BF16), vmem(flat, BF16), vmem(flat, BF16),
            vmem((CELLS, HEADS), F32), vmem((CELLS, HEADS), F32),
            vmem((TEXT, WIDTH), BF16), vmem((TEXT, WIDTH), BF16),
            vmem((8 * (LAST + 1), CELLS), BF16), vmem((CELLS, CELLS), BF16),
            pltpu.SMEM((window_table.shape[2],) + window_table.shape[:2], jnp.int32),
            vmem((16, CELLS), F32), vmem((16, CELLS), F32), vmem((8 * BORROWED, CELLS), F32),
            vmem((2, LAST + 1, 8, WIDTH), BF16), vmem((2, CELLS, WIDTH), BF16),
            vmem((2, BORROWED, 8, WIDTH), BF16), vmem((2, BORROWED, 8, WIDTH), F32),
            vmem((2, 2, 4, 8, WIDTH), F32), vmem((2, 2, 2, 8, WIDTH), F32), vmem((2, 2, 4, 8, WIDTH), F32),
            vmem((2, CELLS // 8, 8, WIDTH), F32), vmem((HEADS, TEXT + CELLS + 8 * BORROWED, CELLS), BF16),
            vmem((2, TILES, 8, HDIM), F32), vmem((TILES, 8, HDIM), F32), vmem((n_x, owned, 8, HDIM), F32),
            vmem((n_x - 1, owned, 8, HDIM), F32), vmem((owned, 8, HDIM), F32), vmem((n_wa, owned, 8, HDIM), F32),
            vmem((owned, 8, HDIM), BF16), vmem((2, n_x, owned, 8, HDIM), BF16),
            dma((11,)), dma((3, CHUNKS)), dma((3, CHUNKS)), dma((CHUNKS,)), dma((CHUNKS,)),
            dma((2, CHUNKS)), dma((2, CHUNKS)), dma((2, CHUNKS)), dma((2, CHUNKS)),
            dma((2,)), dma((2,)), dma((1,)), dma((1,)), dma((2,)), dma((1,)),
            dma((1,)), dma((1,)), dma((1,)), dma((1,)), pltpu.SemaphoreType.REGULAR((2,)), pltpu.SemaphoreType.REGULAR(((n_ha // 4).bit_length(),)),
        ],
        compiler_params=pltpu.CompilerParams(collective_id=0, has_side_effects=True, vmem_limit_bytes=56 << 20),
    )(
        queries.reshape(flat), keys.reshape(flat), values.reshape(flat), out_grad.reshape(flat),
        log_norm.transpose(1, 2, 3, 0).reshape(CELLS, HEADS), delta_rows.transpose(1, 2, 3, 0).reshape(CELLS, HEADS),
        text_keys, text_values, window_table.transpose(2, 0, 1),
        jnp.asarray(order, BF16), jnp.asarray(back, BF16),
    )
    outs = pl.pallas_call(
        store,
        out_shape=[jax.ShapeDtypeStruct(flat, BF16)] * 3 + [jax.ShapeDtypeStruct((TEXT // 8, 8, WIDTH), BF16)] * 2,
        in_specs=[pl.BlockSpec(memory_space=vmem)] * 4,
        out_specs=[hbm] * 5,
        scratch_shapes=[dma((5,))],
        compiler_params=pltpu.CompilerParams(has_side_effects=True, vmem_limit_bytes=1 << 20),
    )(*outs)
    cells = queries.shape
    return (
        outs[0].reshape(cells), outs[1].reshape(cells), outs[2].reshape(cells),
        outs[3].reshape(TEXT, WIDTH), outs[4].reshape(TEXT, WIDTH),
    )


def solution(mesh):
    cells = P("group", "ha", "wa", None)
    stats = P(None, "group", "ha", "wa")
    text = P("group", None)
    return jax.shard_map(
        functools.partial(local, mesh.shape["ha"], mesh.shape["wa"]),
        mesh=mesh,
        in_specs=(cells, cells, cells, cells, stats, stats, text, text, P()),
        out_specs=(cells, cells, cells, text, text),
        check_vma=False,
    )
```

```python
import functools
import math

import jax
import jax.numpy as jnp
import numpy as np
from jax import lax
from jax.experimental import pallas as pl
from jax.experimental.pallas import tpu as pltpu
from jax.sharding import PartitionSpec as P

HEADS = 12
HDIM = 128
TILE = 8
HALO = 2
FRAMES = 2
WIDTH = HEADS * HDIM
CELLS = FRAMES * TILE * TILE
TEXT = 32
CHUNKS = 2
PER_CHUNK = HEADS // CHUNKS
LANES = PER_CHUNK * HDIM
TILES = HEADS * TEXT // 8
SCALE = 1.0 / math.sqrt(HDIM)

TOP, RIGHT, BOTTOM, LEFT, LAST = 4, 7, 10, 13, 16
EAST, UP_RIGHT, DOWN_RIGHT, UP, DOWN, WEST, UP_LEFT, DOWN_LEFT, BORROWED = 0, 4, 5, 6, 10, 14, 18, 19, 20
PARTS = ((0, 6), (6, 14), (14, 20))

F32 = jnp.float32
BF16 = jnp.bfloat16
NT = (((1,), (1,)), ((), ()))
NN = (((1,), (0,)), ((), ()))
TN = (((0,), (0,)), ((), ()))


def dot(left, right, dims, precision=None):
    return lax.dot_general(left, right, dims, precision=precision, preferred_element_type=F32)


def region_rows():
    low, mid, high = range(0, HALO), range(HALO, TILE - HALO), range(TILE - HALO, TILE)
    regions = (
        (mid, mid), (low, low), (low, mid), (low, high), (mid, high),
        (high, high), (high, mid), (high, low), (mid, low), (low, low),
    )
    return [
        (frame * TILE + row) * TILE + col
        for rows, cols in regions
        for frame in range(FRAMES)
        for row in rows
        for col in cols
    ]


def score_grads(key, value, query, cotangent, norm, delta, mask):
    probs = jnp.exp(dot(key, query, NT) * SCALE - norm)
    if mask is not None:
        probs = probs * mask
    score_grad = (probs * (dot(value, cotangent, NT) - delta)).astype(BF16)
    return probs.astype(BF16), score_grad


def kernel(
    n_ha, n_wa,
    q_hbm, k_hbm, v_hbm, o_hbm, norm_hbm, delta_hbm, tk_hbm, tv_hbm, table_hbm, order_hbm, back_hbm,
    dq_out, dk_out, dv_out, text_out,
    q, k, v, o, norm12, delta12, tk, tv, order, back, table,
    norm, delta, mask, packed, own, halo, rim, rows_in, corner_in, cols_in, acc, grads,
    tpart, tsib, tchip, xin, zpart, zin, zall, tfin,
    load_sem, halo_send, halo_recv, rows_send, rows_recv, corner_send, corner_recv, cols_send, cols_recv,
    pair_send, pair_recv, x_send, x_recv, z_send, z_recv, za_send, za_recv, xa_send, xa_recv, ready, met,
):
    n_x = n_ha // 2
    owned = TILES // n_x
    ha, wa = lax.axis_index("ha"), lax.axis_index("wa")
    x, core = ha // 2, ha % 2
    up, down = (ha + n_ha - 1) % n_ha, (ha + 1) % n_ha
    left, right = (wa + n_wa - 1) % n_wa, (wa + 1) % n_wa
    sibling = 2 * x + 1 - core
    distances = [2 ** at for at in range((n_ha // 4).bit_length())]
    far_first = sorted(range(1, n_x), key=lambda step: -min(step, n_x - step))
    half, helper = n_wa // 2, n_wa // 4 + 1
    corner_device = (wa == 0) & (ha == 0)
    first_owner = (wa == 0) & (ha != 0)
    is_owner = first_owner | (wa == 1)
    greeters = jnp.where(ha == 0, 1, 2) - jnp.where(is_owner, 1, 0)

    def remote(src, dst, send, recv, **where):
        return pltpu.make_async_remote_copy(
            src_ref=src, dst_ref=dst, send_sem=send, recv_sem=recv,
            device_id=where, device_id_type=pl.DeviceIdType.MESH,
        )

    def signal(sem, **where):
        pl.semaphore_signal(sem, inc=1, device_id=where, device_id_type=pl.DeviceIdType.MESH)

    def wait_bytes(ref, sem):
        pltpu.make_async_copy(ref, ref, sem).wait()

    def lanes_of(chunk):
        return pl.ds(chunk * LANES, LANES)

    loads = [
        pltpu.make_async_copy(src, dst, load_sem.at[at])
        for at, (src, dst) in enumerate((
            (k_hbm, k), (v_hbm, v), (order_hbm, order), (norm_hbm, norm12), (delta_hbm, delta12),
            (tk_hbm, tk), (tv_hbm, tv), (q_hbm, q), (o_hbm, o), (table_hbm, table), (back_hbm, back),
        ))
    ]
    for load in loads:
        load.start()

    barrier = pltpu.get_barrier_semaphore()
    for col in (left,):
        signal(barrier, wa=col)
        signal(barrier, ha=up, wa=col)
        signal(barrier, ha=down, wa=col)
    signal(barrier, ha=up)
    signal(barrier, ha=down)

    @pl.when(wa != 0)
    def _():
        for step in range(1, n_x):
            signal(barrier, ha=(ha + 2 * step) % n_ha)

    for owner, cond in ((0, first_owner), (1, wa == 1)):

        @pl.when(cond)
        def _():
            for col in range(n_wa):
                if col != owner:
                    signal(barrier, wa=col)

    def send_halo(part, chunk, sends):
        lanes = lanes_of(chunk)
        for src, dst, count, where in sends:
            to_part = [at for at, (low, high) in enumerate(PARTS) if low <= dst < high][0]
            remote(
                packed.at[:, src:src + count, :, lanes], halo.at[:, dst:dst + count, :, lanes],
                halo_send.at[part, chunk], halo_recv.at[to_part, chunk], **where,
            ).start()

    def enter():
        pl.semaphore_wait(barrier, 5 + greeters + jnp.where(wa == 0, 0, n_x - 1))

        @pl.when(wa == 0)
        def _():
            signal(met.at[0], ha=up)
            signal(met.at[0], ha=down)

        signal(ready.at[0], wa=right)
        signal(ready.at[1], ha=up, wa=right)
        signal(ready.at[1], ha=down, wa=right)
        for chunk in range(CHUNKS):
            send_halo(0, chunk, (
                (RIGHT, DOWN_LEFT, 1, {"ha": up, "wa": right}),
                (BOTTOM, UP_LEFT, 1, {"ha": down, "wa": right}),
            ))
        for chunk in range(CHUNKS):
            send_halo(0, chunk, ((RIGHT, WEST, 4, {"wa": right}),))

    def meet_row(at):
        pl.semaphore_wait(met.at[at], 2)
        if at + 1 < len(distances):
            signal(met.at[at + 1], ha=(ha + distances[at + 1]) % n_ha)
            signal(met.at[at + 1], ha=(ha + n_ha - distances[at + 1]) % n_ha)

    def send_rows():
        for chunk in range(CHUNKS):
            send_halo(1, chunk, ((TOP, DOWN, 4, {"ha": up}), (BOTTOM, UP, 4, {"ha": down})))

    def send_west(together):
        side = ((LEFT, EAST, 4, {"wa": left}),)
        corners = (
            (TOP, DOWN_RIGHT, 1, {"ha": up, "wa": left}),
            (LEFT, UP_RIGHT, 1, {"ha": down, "wa": left}),
        )
        pl.semaphore_wait(ready.at[0], 1)
        if together:
            pl.semaphore_wait(ready.at[1], 2)
        for chunk in range(CHUNKS):
            send_halo(2, chunk, corners + side if together else side)
        if not together:
            pl.semaphore_wait(ready.at[1], 2)
            for chunk in range(CHUNKS):
                send_halo(2, chunk, corners)

    for load in loads[0:3]:
        load.wait()
    for at, src in ((0, k), (1, v)):
        for chunk in range(CHUNKS):
            moved = dot(order[...], src[:, lanes_of(chunk)], NN)
            packed[at, :, :, lanes_of(chunk)] = moved.reshape(LAST + 1, 8, LANES).astype(BF16)
            own[at, :, lanes_of(chunk)] = moved[0:CELLS].astype(BF16)

    late = (wa == n_wa - 1) | corner_device
    pl.when(late)(enter)

    for load, src, dst in ((loads[3], norm12, norm), (loads[4], delta12, delta)):
        load.wait()
        dst[0:HEADS, :] = src[...].T

    def statistics(head):
        return norm[head:head + 1, :], delta[head:head + 1, :]

    for load in loads[5:9]:
        load.wait()
    for head in range(HEADS):
        at = pl.ds(head * HDIM, HDIM)
        probs, score_grad = score_grads(tk[:, at], tv[:, at], q[:, at], o[:, at], *statistics(head), None)
        grads[head, 0:TEXT] = score_grad
        tpart[0, 4 * head:4 * head + 4] = (dot(score_grad, q[:, at], NN) * SCALE).reshape(4, 8, HDIM)
        tpart[1, 4 * head:4 * head + 4] = dot(probs, o[:, at], NN).reshape(4, 8, HDIM)

    for load in loads[9:11]:
        load.wait()
    live = [table[block, ha, wa].astype(F32) for block in range(9)]
    for start, count, block in (
        (UP, 4, 1), (UP_LEFT, 1, 0), (UP_RIGHT, 1, 2), (DOWN, 4, 7), (DOWN_LEFT, 1, 6), (DOWN_RIGHT, 1, 8),
        (WEST, 4, 3), (EAST, 4, 5),
    ):
        mask[8 * start:8 * (start + count), :] = jnp.full((8 * count, CELLS), live[block], F32)

    def own_grads():
        for head in range(HEADS):
            at = pl.ds(head * HDIM, HDIM)
            probs, score_grad = score_grads(own[0, :, at], own[1, :, at], q[:, at], o[:, at], *statistics(head), live[4])
            acc[0, :, :, at] = dot(score_grad, q[:, at], NN).reshape(CELLS // 8, 8, HDIM)
            acc[1, :, :, at] = dot(probs, o[:, at], NN).reshape(CELLS // 8, 8, HDIM)
            grads[head, TEXT:TEXT + CELLS] = score_grad

    @pl.when(jnp.logical_not(late))
    def _():
        own_grads()
        enter()

    pair = remote(tpart.at[1 - core], tsib, pair_send.at[0], pair_recv.at[0], ha=sibling)
    pair.start()

    pl.when(jnp.logical_not(late))(send_rows)
    pl.when((wa >= 2) & (wa != n_wa - 1))(lambda: send_west(False))

    @pl.when(wa == 0)
    def _():
        for at in range(len(distances) - 1):
            meet_row(at)
        pl.when(first_owner)(lambda: send_west(True))
        meet_row(len(distances) - 1)

    pair.wait_recv()
    tchip[...] = (tpart[core] + tsib[...]).reshape(n_x, owned, 8, HDIM)
    for step in far_first:
        to = (x + step) % n_x
        remote(tchip.at[to], xin.at[step - 1], x_send.at[0], x_recv.at[0], ha=2 * to + core).start()

    @pl.when(corner_device)
    def _():
        send_rows()
        send_west(True)

    def rim_grads(part, chunk):
        low, high = PARTS[part]
        rows = 8 * (high - low)
        lanes = lanes_of(chunk)
        wait_bytes(halo.at[:, low:high, :, lanes], halo_recv.at[part, chunk])
        for head in range(chunk * PER_CHUNK, (chunk + 1) * PER_CHUNK):
            at = pl.ds(head * HDIM, HDIM)
            key, value = (halo[kind, low:high, :, at].reshape(rows, HDIM) for kind in range(2))
            probs, score_grad = score_grads(
                key, value, q[:, at], o[:, at], *statistics(head), mask[8 * low:8 * high, :]
            )
            rim[0, low:high, :, at] = dot(score_grad, q[:, at], NN).reshape(high - low, 8, HDIM)
            rim[1, low:high, :, at] = dot(probs, o[:, at], NN).reshape(high - low, 8, HDIM)
            grads[head, TEXT + CELLS + 8 * low:TEXT + CELLS + 8 * high] = score_grad

    def corners_out(side, chunk):
        lanes = lanes_of(chunk)
        for source, start, where in ((0, (UP_RIGHT, UP_LEFT)[side], up), (1, (DOWN_RIGHT, DOWN_LEFT)[side], down)):
            remote(
                rim.at[:, start, :, lanes], corner_in.at[side, source, :, :, lanes],
                corner_send.at[side, chunk], corner_recv.at[side, chunk], ha=where,
            ).start()

    def cols_out(side, chunk):
        lanes = lanes_of(chunk)
        wait_bytes(corner_in.at[side, :, :, :, lanes], corner_recv.at[side, chunk])
        start, where = ((EAST, right), (WEST, left))[side]
        below, above = ((start, start + 3), (start + 3, start))[side]
        rim[:, below, :, lanes] += corner_in[side, 0, :, :, lanes]
        rim[:, above, :, lanes] += corner_in[side, 1, :, :, lanes]
        remote(
            rim.at[:, start:start + 4, :, lanes], cols_in.at[side, :, :, :, lanes],
            cols_send.at[side, chunk], cols_recv.at[side, chunk], wa=where,
        ).start()

    def rows_out(chunk):
        lanes = lanes_of(chunk)
        for source, start, where in ((0, UP, up), (1, DOWN, down)):
            remote(
                rim.at[:, start:start + 4, :, lanes], rows_in.at[source, :, :, :, lanes],
                rows_send.at[chunk], rows_recv.at[chunk], ha=where,
            ).start()

    def sum_x():
        wait_bytes(xin, x_recv.at[0])
        total = tchip[x]
        for step in range(n_x - 1):
            total = total + xin[step]
        zpart[...] = total
        for at, cond in enumerate(((wa != 0) & (ha != 0), wa != 1)):

            @pl.when(cond)
            def _():
                remote(zpart, zin.at[wa], z_send.at[at], z_recv.at[0], wa=at).start()

    pl.when(jnp.logical_not(late) & (wa != 0))(sum_x)

    for chunk in range(CHUNKS):
        if chunk == CHUNKS - 1:

            @pl.when(late)
            def _():
                sum_x()
                cols_out(0, 0)

        rim_grads(0, chunk)
        corners_out(0, chunk)

    def east_cols(start):
        for chunk in range(start, CHUNKS):
            cols_out(0, chunk)

    pl.when(wa == n_wa - 1)(send_rows)
    pl.when(jnp.logical_not(late | first_owner))(lambda: east_cols(0))

    @pl.when(late)
    def _():
        east_cols(1)
        own_grads()

    pl.when(wa == n_wa - 1)(lambda: send_west(False))

    for chunk in range(CHUNKS):
        rim_grads(1, chunk)
        rows_out(chunk)

    @pl.when(first_owner)
    def _():
        sum_x()
        east_cols(0)

    pl.when(wa == 1)(lambda: send_west(False))

    def gather_x():
        tfin[core, x] = zall[...]
        for step in far_first:
            to = (x + step) % n_x
            remote(zall, tfin.at[core, x], xa_send.at[0], xa_recv.at[0], ha=2 * to + core).start()

    def sum_z():
        zin[wa] = zpart[...]
        wait_bytes(zin.at[0:n_wa - 1], z_recv.at[0])
        final = zin[0]
        for col in range(1, n_wa):
            final = final + zin[col]
        zall[...] = final.astype(BF16)
        gather_x()

    served = (
        (first_owner, range(half + 2, n_wa), 0),
        ((wa == 1) & (ha != 0), range(2, half + 2), 0),
        ((wa == 1) & (ha == 0), range(2, half + 2), n_x),
        ((wa == helper) & (ha == 0), range(half + 2, n_wa), 0),
    )
    def serve(which):
        for cond, cols, rows in which:

            @pl.when(cond)
            def _():
                for to in range(rows):
                    remote(zall, tfin.at[core, x], za_send.at[0], xa_recv.at[0], ha=2 * to, wa=0).start()
                for col in cols:
                    remote(zall, zall, za_send.at[0], za_recv.at[0], wa=col).start()

    for chunk in range(CHUNKS):
        rim_grads(2, chunk)
        corners_out(1, chunk)

    @pl.when(first_owner)
    def _():
        sum_z()
        serve(served[:1])

    for chunk in range(CHUNKS):
        cols_out(1, chunk)

    @pl.when(wa == 1)
    def _():
        sum_z()
        serve(served[1:3])

    @pl.when(wa >= 2)
    def _():
        wait_bytes(zall, za_recv.at[0])
        gather_x()

    @pl.when(served[3][0])
    def _():
        for col in served[3][1]:
            remote(zall, zall, za_send.at[0], za_recv.at[0], wa=col).start()

    for head in range(HEADS):
        at = pl.ds(head * HDIM, HDIM)
        keys = jnp.concatenate((tk[:, at], own[0, :, at], halo[0, :, :, at].reshape(8 * BORROWED, HDIM)), axis=0)
        dq_out[:, at] = (dot(grads[head], keys, TN) * SCALE).astype(BF16)

    for chunk in range(CHUNKS):
        lanes = lanes_of(chunk)
        wait_bytes(rows_in.at[:, :, :, :, lanes], rows_recv.at[chunk])
        acc[:, BOTTOM:BOTTOM + 4, :, lanes] += rows_in[0, :, :, :, lanes]
        acc[:, TOP:TOP + 4, :, lanes] += rows_in[1, :, :, :, lanes]
        wait_bytes(cols_in.at[1, :, :, :, lanes], cols_recv.at[1, chunk])
        acc[:, RIGHT:RIGHT + 4, :, lanes] += cols_in[1, :, :, :, lanes]
        wait_bytes(cols_in.at[0, :, :, :, lanes], cols_recv.at[0, chunk])
        acc[:, LEFT:LEFT + 3, :, lanes] += cols_in[0, :, 0:3, :, lanes]
        acc[:, TOP, :, lanes] += cols_in[0, :, 3, :, lanes]
        for at, out, factor in ((0, dk_out, SCALE), (1, dv_out, 1.0)):
            total = (acc[at, :, :, lanes] * factor).reshape(CELLS, LANES).astype(BF16)
            out[:, lanes] = dot(back[...], total, NN).astype(BF16)

    @pl.when(corner_device)
    def _():
        wait_bytes(tfin.at[core], xa_recv.at[0])

    @pl.when(jnp.logical_not(corner_device))
    def _():
        wait_bytes(tfin.at[core, 0:n_x - 1], xa_recv.at[0])

    last = remote(tfin.at[core], tfin.at[core], pair_send.at[1], pair_recv.at[1], ha=sibling)
    last.start()
    wait_bytes(tfin.at[1 - core], pair_recv.at[1])
    for at in range(2):
        for tile in range(TILES):
            text_out[at, tile % 4, :, (tile // 4) * HDIM:(tile // 4 + 1) * HDIM] = tfin[at, tile // owned, tile % owned]

    last.wait_send()
    pair.wait_send()
    for chunk in range(CHUNKS):
        lanes = lanes_of(chunk)
        for part, (low, high) in enumerate(PARTS):
            wait_bytes(halo.at[:, low:high, :, lanes], halo_send.at[part, chunk])
        wait_bytes(rows_in.at[:, :, :, :, lanes], rows_send.at[chunk])
        for side in range(2):
            wait_bytes(corner_in.at[side, :, :, :, lanes], corner_send.at[side, chunk])
            wait_bytes(cols_in.at[side, :, :, :, lanes], cols_send.at[side, chunk])
    wait_bytes(xin, x_send.at[0])

    for at, cond in enumerate(((wa != 0) & (ha != 0), wa != 1)):

        @pl.when(cond)
        def _():
            wait_bytes(zpart, z_send.at[at])

    for cond, cols, rows in served:

        @pl.when(cond)
        def _():
            wait_bytes(zin.at[0:(len(cols) + rows) // 2], za_send.at[0])

    @pl.when(jnp.logical_not(corner_device))
    def _():
        wait_bytes(tfin.at[core, 0:n_x - 1], xa_send.at[0])


def store(dq, dk, dv, text, dq_hbm, dk_hbm, dv_hbm, dtk_hbm, dtv_hbm, sem):
    copies = [
        pltpu.make_async_copy(src, dst, sem.at[at])
        for at, (src, dst) in enumerate((
            (dq, dq_hbm), (dk, dk_hbm), (dv, dv_hbm), (text.at[0], dtk_hbm), (text.at[1], dtv_hbm),
        ))
    ]
    for copy in copies:
        copy.start()
    for copy in copies:
        copy.wait()


def local(n_ha, n_wa, queries, keys, values, out_grad, log_norm, delta_rows, text_keys, text_values, window_table):
    n_x = n_ha // 2
    owned = TILES // n_x
    rows = region_rows()
    order = np.zeros((8 * (LAST + 1), CELLS), np.float32)
    order[np.arange(len(rows)), rows] = 1.0
    back = order[:CELLS].T
    hbm = pl.BlockSpec(memory_space=pl.ANY)
    vmem = pltpu.VMEM
    dma = pltpu.SemaphoreType.DMA
    flat = (CELLS, WIDTH)
    outs = pl.pallas_call(
        functools.partial(kernel, n_ha, n_wa),
        out_shape=[vmem(flat, BF16)] * 3 + [vmem((2, TEXT // 8, 8, WIDTH), BF16)],
        in_specs=[hbm] * 11,
        out_specs=[pl.BlockSpec(memory_space=vmem)] * 4,
        scratch_shapes=[
            vmem(flat, BF16), vmem(flat, BF16), vmem(flat, BF16), vmem(flat, BF16),
            vmem((CELLS, HEADS), F32), vmem((CELLS, HEADS), F32),
            vmem((TEXT, WIDTH), BF16), vmem((TEXT, WIDTH), BF16),
            vmem((8 * (LAST + 1), CELLS), BF16), vmem((CELLS, CELLS), BF16),
            pltpu.SMEM((window_table.shape[2],) + window_table.shape[:2], jnp.int32),
            vmem((16, CELLS), F32), vmem((16, CELLS), F32), vmem((8 * BORROWED, CELLS), F32),
            vmem((2, LAST + 1, 8, WIDTH), BF16), vmem((2, CELLS, WIDTH), BF16),
            vmem((2, BORROWED, 8, WIDTH), BF16), vmem((2, BORROWED, 8, WIDTH), F32),
            vmem((2, 2, 4, 8, WIDTH), F32), vmem((2, 2, 2, 8, WIDTH), F32), vmem((2, 2, 4, 8, WIDTH), F32),
            vmem((2, CELLS // 8, 8, WIDTH), F32), vmem((HEADS, TEXT + CELLS + 8 * BORROWED, CELLS), BF16),
            vmem((2, TILES, 8, HDIM), F32), vmem((TILES, 8, HDIM), F32), vmem((n_x, owned, 8, HDIM), F32),
            vmem((n_x - 1, owned, 8, HDIM), F32), vmem((owned, 8, HDIM), F32), vmem((n_wa, owned, 8, HDIM), F32),
            vmem((owned, 8, HDIM), BF16), vmem((2, n_x, owned, 8, HDIM), BF16),
            dma((11,)), dma((3, CHUNKS)), dma((3, CHUNKS)), dma((CHUNKS,)), dma((CHUNKS,)),
            dma((2, CHUNKS)), dma((2, CHUNKS)), dma((2, CHUNKS)), dma((2, CHUNKS)),
            dma((2,)), dma((2,)), dma((1,)), dma((1,)), dma((2,)), dma((1,)),
            dma((1,)), dma((1,)), dma((1,)), dma((1,)), pltpu.SemaphoreType.REGULAR((2,)), pltpu.SemaphoreType.REGULAR(((n_ha // 4).bit_length(),)),
        ],
        compiler_params=pltpu.CompilerParams(collective_id=0, has_side_effects=True, vmem_limit_bytes=56 << 20),
    )(
        queries.reshape(flat), keys.reshape(flat), values.reshape(flat), out_grad.reshape(flat),
        log_norm.transpose(1, 2, 3, 0).reshape(CELLS, HEADS), delta_rows.transpose(1, 2, 3, 0).reshape(CELLS, HEADS),
        text_keys, text_values, window_table.transpose(2, 0, 1),
        jnp.asarray(order, BF16), jnp.asarray(back, BF16),
    )
    outs = pl.pallas_call(
        store,
        out_shape=[jax.ShapeDtypeStruct(flat, BF16)] * 3 + [jax.ShapeDtypeStruct((TEXT // 8, 8, WIDTH), BF16)] * 2,
        in_specs=[pl.BlockSpec(memory_space=vmem)] * 4,
        out_specs=[hbm] * 5,
        scratch_shapes=[dma((5,))],
        compiler_params=pltpu.CompilerParams(has_side_effects=True, vmem_limit_bytes=1 << 20),
    )(*outs)
    cells = queries.shape
    return (
        outs[0].reshape(cells), outs[1].reshape(cells), outs[2].reshape(cells),
        outs[3].reshape(TEXT, WIDTH), outs[4].reshape(TEXT, WIDTH),
    )


def solution(mesh):
    cells = P("group", "ha", "wa", None)
    stats = P(None, "group", "ha", "wa")
    text = P("group", None)
    return jax.shard_map(
        functools.partial(local, mesh.shape["ha"], mesh.shape["wa"]),
        mesh=mesh,
        in_specs=(cells, cells, cells, cells, stats, stats, text, text, P()),
        out_specs=(cells, cells, cells, text, text),
        check_vma=False,
    )
```

```python
import functools
import math

import jax
import jax.numpy as jnp
import numpy as np
from jax import lax
from jax.experimental import pallas as pl
from jax.experimental.pallas import tpu as pltpu
from jax.sharding import PartitionSpec as P

HEADS = 12
HDIM = 128
TILE = 8
HALO = 2
FRAMES = 2
WIDTH = HEADS * HDIM
CELLS = FRAMES * TILE * TILE
TEXT = 32
CHUNKS = 2
PER_CHUNK = HEADS // CHUNKS
LANES = PER_CHUNK * HDIM
TILES = HEADS * TEXT // 8
SCALE = 1.0 / math.sqrt(HDIM)

TOP, RIGHT, BOTTOM, LEFT, LAST = 4, 7, 10, 13, 16
EAST, UP_RIGHT, DOWN_RIGHT, UP, DOWN, WEST, UP_LEFT, DOWN_LEFT, BORROWED = 0, 4, 5, 6, 10, 14, 18, 19, 20
PARTS = ((0, 6), (6, 14), (14, 20))

F32 = jnp.float32
BF16 = jnp.bfloat16
NT = (((1,), (1,)), ((), ()))
NN = (((1,), (0,)), ((), ()))
TN = (((0,), (0,)), ((), ()))


def dot(left, right, dims, precision=None):
    return lax.dot_general(left, right, dims, precision=precision, preferred_element_type=F32)


def region_rows():
    low, mid, high = range(0, HALO), range(HALO, TILE - HALO), range(TILE - HALO, TILE)
    regions = (
        (mid, mid), (low, low), (low, mid), (low, high), (mid, high),
        (high, high), (high, mid), (high, low), (mid, low), (low, low),
    )
    return [
        (frame * TILE + row) * TILE + col
        for rows, cols in regions
        for frame in range(FRAMES)
        for row in rows
        for col in cols
    ]


def score_grads(key, value, query, cotangent, norm, delta, mask):
    probs = jnp.exp(dot(key, query, NT) * SCALE - norm)
    if mask is not None:
        probs = probs * mask
    score_grad = (probs * (dot(value, cotangent, NT) - delta)).astype(BF16)
    return probs.astype(BF16), score_grad


def kernel(
    n_ha, n_wa,
    q_hbm, k_hbm, v_hbm, o_hbm, norm_hbm, delta_hbm, tk_hbm, tv_hbm, table_hbm, order_hbm, back_hbm,
    dq_out, dk_out, dv_out, text_out,
    q, k, v, o, norm12, delta12, tk, tv, order, back, table,
    norm, delta, mask, packed, own, halo, rim, rows_in, corner_in, cols_in, acc, grads,
    tpart, tsib, tchip, xin, zpart, zin, zall, tfin,
    load_sem, halo_send, halo_recv, rows_send, rows_recv, corner_send, corner_recv, cols_send, cols_recv,
    pair_send, pair_recv, x_send, x_recv, z_send, z_recv, za_send, za_recv, xa_send, xa_recv, ready, met,
):
    n_x = n_ha // 2
    owned = TILES // n_x
    ha, wa = lax.axis_index("ha"), lax.axis_index("wa")
    x, core = ha // 2, ha % 2
    up, down = (ha + n_ha - 1) % n_ha, (ha + 1) % n_ha
    left, right = (wa + n_wa - 1) % n_wa, (wa + 1) % n_wa
    sibling = 2 * x + 1 - core
    distances = [2 ** at for at in range((n_ha // 4).bit_length())]
    far_first = sorted(range(1, n_x), key=lambda step: -min(step, n_x - step))
    half, helper = n_wa // 2, n_wa // 4 + 1
    corner_device = (wa == 0) & (ha == 0)
    first_owner = (wa == 0) & (ha != 0)
    meets = (wa == 0) | (wa == n_wa - 1)
    is_owner = first_owner | (wa == 1)
    greeters = jnp.where(ha == 0, 1, 2) - jnp.where(is_owner, 1, 0)

    def remote(src, dst, send, recv, **where):
        return pltpu.make_async_remote_copy(
            src_ref=src, dst_ref=dst, send_sem=send, recv_sem=recv,
            device_id=where, device_id_type=pl.DeviceIdType.MESH,
        )

    def signal(sem, **where):
        pl.semaphore_signal(sem, inc=1, device_id=where, device_id_type=pl.DeviceIdType.MESH)

    def wait_bytes(ref, sem):
        pltpu.make_async_copy(ref, ref, sem).wait()

    def lanes_of(chunk):
        return pl.ds(chunk * LANES, LANES)

    loads = [
        pltpu.make_async_copy(src, dst, load_sem.at[at])
        for at, (src, dst) in enumerate((
            (k_hbm, k), (v_hbm, v), (order_hbm, order), (norm_hbm, norm12), (delta_hbm, delta12),
            (tk_hbm, tk), (tv_hbm, tv), (q_hbm, q), (o_hbm, o), (table_hbm, table), (back_hbm, back),
        ))
    ]
    for load in loads:
        load.start()

    barrier = pltpu.get_barrier_semaphore()
    for col in (left,):
        signal(barrier, wa=col)
        signal(barrier, ha=up, wa=col)
        signal(barrier, ha=down, wa=col)
    signal(barrier, ha=up)
    signal(barrier, ha=down)

    @pl.when(jnp.logical_not(meets))
    def _():
        for step in range(1, n_x):
            signal(barrier, ha=(ha + 2 * step) % n_ha)

    for owner, cond in ((0, first_owner), (1, wa == 1)):

        @pl.when(cond)
        def _():
            for col in range(n_wa):
                if col != owner:
                    signal(barrier, wa=col)

    def send_halo(part, chunk, sends):
        lanes = lanes_of(chunk)
        for src, dst, count, where in sends:
            to_part = [at for at, (low, high) in enumerate(PARTS) if low <= dst < high][0]
            remote(
                packed.at[:, src:src + count, :, lanes], halo.at[:, dst:dst + count, :, lanes],
                halo_send.at[part, chunk], halo_recv.at[to_part, chunk], **where,
            ).start()

    def enter():
        pl.semaphore_wait(barrier, 5 + greeters + jnp.where(meets, 0, n_x - 1))

        @pl.when(meets)
        def _():
            signal(met.at[0], ha=up)
            signal(met.at[0], ha=down)

        signal(ready.at[0], wa=right)
        signal(ready.at[1], ha=up, wa=right)
        signal(ready.at[1], ha=down, wa=right)
        for chunk in range(CHUNKS):
            send_halo(0, chunk, (
                (RIGHT, DOWN_LEFT, 1, {"ha": up, "wa": right}),
                (BOTTOM, UP_LEFT, 1, {"ha": down, "wa": right}),
            ))
        for chunk in range(CHUNKS):
            send_halo(0, chunk, ((RIGHT, WEST, 4, {"wa": right}),))

    def meet_row(at):
        pl.semaphore_wait(met.at[at], 2)
        if at + 1 < len(distances):
            signal(met.at[at + 1], ha=(ha + distances[at + 1]) % n_ha)
            signal(met.at[at + 1], ha=(ha + n_ha - distances[at + 1]) % n_ha)

    def send_rows():
        for chunk in range(CHUNKS):
            send_halo(1, chunk, ((TOP, DOWN, 4, {"ha": up}), (BOTTOM, UP, 4, {"ha": down})))

    def send_west(together):
        side = ((LEFT, EAST, 4, {"wa": left}),)
        corners = (
            (TOP, DOWN_RIGHT, 1, {"ha": up, "wa": left}),
            (LEFT, UP_RIGHT, 1, {"ha": down, "wa": left}),
        )
        pl.semaphore_wait(ready.at[0], 1)
        if together:
            pl.semaphore_wait(ready.at[1], 2)
        for chunk in range(CHUNKS):
            send_halo(2, chunk, corners + side if together else side)
        if not together:
            pl.semaphore_wait(ready.at[1], 2)
            for chunk in range(CHUNKS):
                send_halo(2, chunk, corners)

    for load in loads[0:3]:
        load.wait()
    for at, src in ((0, k), (1, v)):
        for chunk in range(CHUNKS):
            moved = dot(order[...], src[:, lanes_of(chunk)], NN)
            packed[at, :, :, lanes_of(chunk)] = moved.reshape(LAST + 1, 8, LANES).astype(BF16)
            own[at, :, lanes_of(chunk)] = moved[0:CELLS].astype(BF16)

    late = (wa == n_wa - 1) | corner_device
    pl.when(late)(enter)

    for load, src, dst in ((loads[3], norm12, norm), (loads[4], delta12, delta)):
        load.wait()
        dst[0:HEADS, :] = src[...].T

    def statistics(head):
        return norm[head:head + 1, :], delta[head:head + 1, :]

    for load in loads[5:9]:
        load.wait()
    for head in range(HEADS):
        at = pl.ds(head * HDIM, HDIM)
        probs, score_grad = score_grads(tk[:, at], tv[:, at], q[:, at], o[:, at], *statistics(head), None)
        grads[head, 0:TEXT] = score_grad
        tpart[0, 4 * head:4 * head + 4] = (dot(score_grad, q[:, at], NN) * SCALE).reshape(4, 8, HDIM)
        tpart[1, 4 * head:4 * head + 4] = dot(probs, o[:, at], NN).reshape(4, 8, HDIM)

    for load in loads[9:11]:
        load.wait()
    live = [table[block, ha, wa].astype(F32) for block in range(9)]
    for start, count, block in (
        (UP, 4, 1), (UP_LEFT, 1, 0), (UP_RIGHT, 1, 2), (DOWN, 4, 7), (DOWN_LEFT, 1, 6), (DOWN_RIGHT, 1, 8),
        (WEST, 4, 3), (EAST, 4, 5),
    ):
        mask[8 * start:8 * (start + count), :] = jnp.full((8 * count, CELLS), live[block], F32)

    def own_grads():
        for head in range(HEADS):
            at = pl.ds(head * HDIM, HDIM)
            probs, score_grad = score_grads(own[0, :, at], own[1, :, at], q[:, at], o[:, at], *statistics(head), live[4])
            acc[0, :, :, at] = dot(score_grad, q[:, at], NN).reshape(CELLS // 8, 8, HDIM)
            acc[1, :, :, at] = dot(probs, o[:, at], NN).reshape(CELLS // 8, 8, HDIM)
            grads[head, TEXT:TEXT + CELLS] = score_grad

    @pl.when(jnp.logical_not(late))
    def _():
        own_grads()
        enter()

    pair = remote(tpart.at[1 - core], tsib, pair_send.at[0], pair_recv.at[0], ha=sibling)
    pair.start()

    pl.when(jnp.logical_not(late))(send_rows)
    pl.when((wa >= 2) & (wa != n_wa - 1))(lambda: send_west(False))

    @pl.when(meets)
    def _():
        for at in range(len(distances) - 1):
            meet_row(at)
        pl.when(first_owner)(lambda: send_west(True))
        meet_row(len(distances) - 1)

    pair.wait_recv()
    tchip[...] = (tpart[core] + tsib[...]).reshape(n_x, owned, 8, HDIM)
    for step in far_first:
        to = (x + step) % n_x
        remote(tchip.at[to], xin.at[step - 1], x_send.at[0], x_recv.at[0], ha=2 * to + core).start()

    @pl.when(corner_device)
    def _():
        send_rows()
        send_west(True)

    def rim_grads(part, chunk):
        low, high = PARTS[part]
        rows = 8 * (high - low)
        lanes = lanes_of(chunk)
        wait_bytes(halo.at[:, low:high, :, lanes], halo_recv.at[part, chunk])
        for head in range(chunk * PER_CHUNK, (chunk + 1) * PER_CHUNK):
            at = pl.ds(head * HDIM, HDIM)
            key, value = (halo[kind, low:high, :, at].reshape(rows, HDIM) for kind in range(2))
            probs, score_grad = score_grads(
                key, value, q[:, at], o[:, at], *statistics(head), mask[8 * low:8 * high, :]
            )
            rim[0, low:high, :, at] = dot(score_grad, q[:, at], NN).reshape(high - low, 8, HDIM)
            rim[1, low:high, :, at] = dot(probs, o[:, at], NN).reshape(high - low, 8, HDIM)
            grads[head, TEXT + CELLS + 8 * low:TEXT + CELLS + 8 * high] = score_grad

    def corners_out(side, chunk):
        lanes = lanes_of(chunk)
        for source, start, where in ((0, (UP_RIGHT, UP_LEFT)[side], up), (1, (DOWN_RIGHT, DOWN_LEFT)[side], down)):
            remote(
                rim.at[:, start, :, lanes], corner_in.at[side, source, :, :, lanes],
                corner_send.at[side, chunk], corner_recv.at[side, chunk], ha=where,
            ).start()

    def cols_out(side, chunk):
        lanes = lanes_of(chunk)
        wait_bytes(corner_in.at[side, :, :, :, lanes], corner_recv.at[side, chunk])
        start, where = ((EAST, right), (WEST, left))[side]
        below, above = ((start, start + 3), (start + 3, start))[side]
        rim[:, below, :, lanes] += corner_in[side, 0, :, :, lanes]
        rim[:, above, :, lanes] += corner_in[side, 1, :, :, lanes]
        remote(
            rim.at[:, start:start + 4, :, lanes], cols_in.at[side, :, :, :, lanes],
            cols_send.at[side, chunk], cols_recv.at[side, chunk], wa=where,
        ).start()

    def rows_out(chunk):
        lanes = lanes_of(chunk)
        for source, start, where in ((0, UP, up), (1, DOWN, down)):
            remote(
                rim.at[:, start:start + 4, :, lanes], rows_in.at[source, :, :, :, lanes],
                rows_send.at[chunk], rows_recv.at[chunk], ha=where,
            ).start()

    def sum_x():
        wait_bytes(xin, x_recv.at[0])
        total = tchip[x]
        for step in range(n_x - 1):
            total = total + xin[step]
        zpart[...] = total
        for at, cond in enumerate(((wa != 0) & (ha != 0), wa != 1)):

            @pl.when(cond)
            def _():
                remote(zpart, zin.at[wa], z_send.at[at], z_recv.at[0], wa=at).start()

    pl.when(jnp.logical_not(late) & (wa != 0))(sum_x)

    for chunk in range(CHUNKS):
        if chunk == CHUNKS - 1:

            @pl.when(late)
            def _():
                sum_x()
                cols_out(0, 0)

        rim_grads(0, chunk)
        corners_out(0, chunk)

    def east_cols(start):
        for chunk in range(start, CHUNKS):
            cols_out(0, chunk)

    pl.when(wa == n_wa - 1)(send_rows)
    pl.when(jnp.logical_not(late | first_owner))(lambda: east_cols(0))

    @pl.when(late)
    def _():
        east_cols(1)
        own_grads()

    pl.when(wa == n_wa - 1)(lambda: send_west(False))

    for chunk in range(CHUNKS):
        rim_grads(1, chunk)
        rows_out(chunk)

    @pl.when(first_owner)
    def _():
        sum_x()
        east_cols(0)

    pl.when(wa == 1)(lambda: send_west(False))

    def gather_x():
        tfin[core, x] = zall[...]
        for step in far_first:
            to = (x + step) % n_x
            remote(zall, tfin.at[core, x], xa_send.at[0], xa_recv.at[0], ha=2 * to + core).start()

    def sum_z():
        zin[wa] = zpart[...]
        wait_bytes(zin.at[0:n_wa - 1], z_recv.at[0])
        final = zin[0]
        for col in range(1, n_wa):
            final = final + zin[col]
        zall[...] = final.astype(BF16)
        gather_x()

    served = (
        (first_owner, range(half + 2, n_wa), 0),
        ((wa == 1) & (ha != 0), range(2, half + 2), 0),
        ((wa == 1) & (ha == 0), range(2, half + 2), n_x),
        ((wa == helper) & (ha == 0), range(half + 2, n_wa), 0),
    )
    def serve(which):
        for cond, cols, rows in which:

            @pl.when(cond)
            def _():
                for to in range(rows):
                    remote(zall, tfin.at[core, x], za_send.at[0], xa_recv.at[0], ha=2 * to, wa=0).start()
                for col in cols:
                    remote(zall, zall, za_send.at[0], za_recv.at[0], wa=col).start()

    for chunk in range(CHUNKS):
        rim_grads(2, chunk)
        corners_out(1, chunk)

    @pl.when(first_owner)
    def _():
        sum_z()
        serve(served[:1])

    for chunk in range(CHUNKS):
        cols_out(1, chunk)

    @pl.when(wa == 1)
    def _():
        sum_z()
        serve(served[1:3])

    @pl.when(wa >= 2)
    def _():
        wait_bytes(zall, za_recv.at[0])
        gather_x()

    @pl.when(served[3][0])
    def _():
        for col in served[3][1]:
            remote(zall, zall, za_send.at[0], za_recv.at[0], wa=col).start()

    for head in range(HEADS):
        at = pl.ds(head * HDIM, HDIM)
        keys = jnp.concatenate((tk[:, at], own[0, :, at], halo[0, :, :, at].reshape(8 * BORROWED, HDIM)), axis=0)
        dq_out[:, at] = (dot(grads[head], keys, TN) * SCALE).astype(BF16)

    for chunk in range(CHUNKS):
        lanes = lanes_of(chunk)
        wait_bytes(rows_in.at[:, :, :, :, lanes], rows_recv.at[chunk])
        acc[:, BOTTOM:BOTTOM + 4, :, lanes] += rows_in[0, :, :, :, lanes]
        acc[:, TOP:TOP + 4, :, lanes] += rows_in[1, :, :, :, lanes]
        wait_bytes(cols_in.at[1, :, :, :, lanes], cols_recv.at[1, chunk])
        acc[:, RIGHT:RIGHT + 4, :, lanes] += cols_in[1, :, :, :, lanes]
        wait_bytes(cols_in.at[0, :, :, :, lanes], cols_recv.at[0, chunk])
        acc[:, LEFT:LEFT + 3, :, lanes] += cols_in[0, :, 0:3, :, lanes]
        acc[:, TOP, :, lanes] += cols_in[0, :, 3, :, lanes]
        for at, out, factor in ((0, dk_out, SCALE), (1, dv_out, 1.0)):
            total = (acc[at, :, :, lanes] * factor).reshape(CELLS, LANES).astype(BF16)
            out[:, lanes] = dot(back[...], total, NN).astype(BF16)

    @pl.when(corner_device)
    def _():
        wait_bytes(tfin.at[core], xa_recv.at[0])

    @pl.when(jnp.logical_not(corner_device))
    def _():
        wait_bytes(tfin.at[core, 0:n_x - 1], xa_recv.at[0])

    last = remote(tfin.at[core], tfin.at[core], pair_send.at[1], pair_recv.at[1], ha=sibling)
    last.start()
    wait_bytes(tfin.at[1 - core], pair_recv.at[1])
    for at in range(2):
        for tile in range(TILES):
            text_out[at, tile % 4, :, (tile // 4) * HDIM:(tile // 4 + 1) * HDIM] = tfin[at, tile // owned, tile % owned]

    last.wait_send()
    pair.wait_send()
    for chunk in range(CHUNKS):
        lanes = lanes_of(chunk)
        for part, (low, high) in enumerate(PARTS):
            wait_bytes(halo.at[:, low:high, :, lanes], halo_send.at[part, chunk])
        wait_bytes(rows_in.at[:, :, :, :, lanes], rows_send.at[chunk])
        for side in range(2):
            wait_bytes(corner_in.at[side, :, :, :, lanes], corner_send.at[side, chunk])
            wait_bytes(cols_in.at[side, :, :, :, lanes], cols_send.at[side, chunk])
    wait_bytes(xin, x_send.at[0])

    for at, cond in enumerate(((wa != 0) & (ha != 0), wa != 1)):

        @pl.when(cond)
        def _():
            wait_bytes(zpart, z_send.at[at])

    for cond, cols, rows in served:

        @pl.when(cond)
        def _():
            wait_bytes(zin.at[0:(len(cols) + rows) // 2], za_send.at[0])

    @pl.when(jnp.logical_not(corner_device))
    def _():
        wait_bytes(tfin.at[core, 0:n_x - 1], xa_send.at[0])


def store(dq, dk, dv, text, dq_hbm, dk_hbm, dv_hbm, dtk_hbm, dtv_hbm, sem):
    copies = [
        pltpu.make_async_copy(src, dst, sem.at[at])
        for at, (src, dst) in enumerate((
            (dq, dq_hbm), (dk, dk_hbm), (dv, dv_hbm), (text.at[0], dtk_hbm), (text.at[1], dtv_hbm),
        ))
    ]
    for copy in copies:
        copy.start()
    for copy in copies:
        copy.wait()


def local(n_ha, n_wa, queries, keys, values, out_grad, log_norm, delta_rows, text_keys, text_values, window_table):
    n_x = n_ha // 2
    owned = TILES // n_x
    rows = region_rows()
    order = np.zeros((8 * (LAST + 1), CELLS), np.float32)
    order[np.arange(len(rows)), rows] = 1.0
    back = order[:CELLS].T
    hbm = pl.BlockSpec(memory_space=pl.ANY)
    vmem = pltpu.VMEM
    dma = pltpu.SemaphoreType.DMA
    flat = (CELLS, WIDTH)
    outs = pl.pallas_call(
        functools.partial(kernel, n_ha, n_wa),
        out_shape=[vmem(flat, BF16)] * 3 + [vmem((2, TEXT // 8, 8, WIDTH), BF16)],
        in_specs=[hbm] * 11,
        out_specs=[pl.BlockSpec(memory_space=vmem)] * 4,
        scratch_shapes=[
            vmem(flat, BF16), vmem(flat, BF16), vmem(flat, BF16), vmem(flat, BF16),
            vmem((CELLS, HEADS), F32), vmem((CELLS, HEADS), F32),
            vmem((TEXT, WIDTH), BF16), vmem((TEXT, WIDTH), BF16),
            vmem((8 * (LAST + 1), CELLS), BF16), vmem((CELLS, CELLS), BF16),
            pltpu.SMEM((window_table.shape[2],) + window_table.shape[:2], jnp.int32),
            vmem((16, CELLS), F32), vmem((16, CELLS), F32), vmem((8 * BORROWED, CELLS), F32),
            vmem((2, LAST + 1, 8, WIDTH), BF16), vmem((2, CELLS, WIDTH), BF16),
            vmem((2, BORROWED, 8, WIDTH), BF16), vmem((2, BORROWED, 8, WIDTH), F32),
            vmem((2, 2, 4, 8, WIDTH), F32), vmem((2, 2, 2, 8, WIDTH), F32), vmem((2, 2, 4, 8, WIDTH), F32),
            vmem((2, CELLS // 8, 8, WIDTH), F32), vmem((HEADS, TEXT + CELLS + 8 * BORROWED, CELLS), BF16),
            vmem((2, TILES, 8, HDIM), F32), vmem((TILES, 8, HDIM), F32), vmem((n_x, owned, 8, HDIM), F32),
            vmem((n_x - 1, owned, 8, HDIM), F32), vmem((owned, 8, HDIM), F32), vmem((n_wa, owned, 8, HDIM), F32),
            vmem((owned, 8, HDIM), BF16), vmem((2, n_x, owned, 8, HDIM), BF16),
            dma((11,)), dma((3, CHUNKS)), dma((3, CHUNKS)), dma((CHUNKS,)), dma((CHUNKS,)),
            dma((2, CHUNKS)), dma((2, CHUNKS)), dma((2, CHUNKS)), dma((2, CHUNKS)),
            dma((2,)), dma((2,)), dma((1,)), dma((1,)), dma((2,)), dma((1,)),
            dma((1,)), dma((1,)), dma((1,)), dma((1,)), pltpu.SemaphoreType.REGULAR((2,)), pltpu.SemaphoreType.REGULAR(((n_ha // 4).bit_length(),)),
        ],
        compiler_params=pltpu.CompilerParams(collective_id=0, has_side_effects=True, vmem_limit_bytes=56 << 20),
    )(
        queries.reshape(flat), keys.reshape(flat), values.reshape(flat), out_grad.reshape(flat),
        log_norm.transpose(1, 2, 3, 0).reshape(CELLS, HEADS), delta_rows.transpose(1, 2, 3, 0).reshape(CELLS, HEADS),
        text_keys, text_values, window_table.transpose(2, 0, 1),
        jnp.asarray(order, BF16), jnp.asarray(back, BF16),
    )
    outs = pl.pallas_call(
        store,
        out_shape=[jax.ShapeDtypeStruct(flat, BF16)] * 3 + [jax.ShapeDtypeStruct((TEXT // 8, 8, WIDTH), BF16)] * 2,
        in_specs=[pl.BlockSpec(memory_space=vmem)] * 4,
        out_specs=[hbm] * 5,
        scratch_shapes=[dma((5,))],
        compiler_params=pltpu.CompilerParams(has_side_effects=True, vmem_limit_bytes=1 << 20),
    )(*outs)
    cells = queries.shape
    return (
        outs[0].reshape(cells), outs[1].reshape(cells), outs[2].reshape(cells),
        outs[3].reshape(TEXT, WIDTH), outs[4].reshape(TEXT, WIDTH),
    )


def solution(mesh):
    cells = P("group", "ha", "wa", None)
    stats = P(None, "group", "ha", "wa")
    text = P("group", None)
    return jax.shard_map(
        functools.partial(local, mesh.shape["ha"], mesh.shape["wa"]),
        mesh=mesh,
        in_specs=(cells, cells, cells, cells, stats, stats, text, text, P()),
        out_specs=(cells, cells, cells, text, text),
        check_vma=False,
    )
```
